32 devices in a mesh: row: 4 (over y, x), col: 8 (over z, core).
Axes of the slice: x: 2, y: 2, z: 4, core: 2. Of those that a mesh axis runs over, the one named last changes fastest.
Arguments:
- e_field: float32 [3, 64, 32, 1024], P(None, None, 'row', 'col'), may hold values from -6 to 6
- h_field: float32 [3, 64, 32, 1024], P(None, None, 'row', 'col'), may hold values from -6 to 6
- e_coef: float32 [64, 32, 1024], P(None, 'row', 'col'), may hold values from 0.125 to 0.5
- basis: float32 [128, 32, 1024], P('row', None, 'col'), may hold values from -0.03125 to 0.03125
- pml_width: int32 [4], replicated, may hold values from 2 to 8
- snap_index: int32 [64], replicated, may hold values from 0 to 383
Outputs:
- e_final: float32 [3, 64, 32, 1024], P(None, None, 'row', 'col')
- h_final: float32 [3, 64, 32, 1024], P(None, None, 'row', 'col')
- coefficients: float32 [64, 128], replicated
- gram: float32 [64, 64], replicated
The draws below stay inside these ranges and needn't reach their ends.
All inputs are finite; a program needn't handle non-finite values.
Results may differ from the reference program's by a relative error of at most 0.00008.
Values sent between devices are 32-bit elements; how exact they have to be, the bound alone decides.
A program may use at most 64 MiB of HBM per device.

```python
import math
import jax
import jax.numpy as jnp
from jax import lax

NZ = 64
STEPS = 8
RANK = 128
SNAPS = 64
NX = 32
NY = 1024


def place_ends(entries, own_key, low, high):
    spot = [jax.random.randint(jax.random.fold_in(own_key, axis), (), 0, length) for axis, length in enumerate(entries.shape)]
    main_axis = entries.shape.index(max(entries.shape))
    next_to = spot[:main_axis] + [(spot[main_axis] + 1) % entries.shape[main_axis]] + spot[main_axis + 1:]
    return entries.at[tuple(spot)].set(low).at[tuple(next_to)].set(high)


def level_of(rng, shape, shards, smallest, top_value):
    level, own = 1.0, jax.random.fold_in(rng, 6)
    for position, blocks in shards:
        draws = jnp.exp(jax.random.uniform(jax.random.fold_in(own, position), (blocks,), jnp.float32, smallest / len(shards), top_value / len(shards)))
        level = level * jnp.repeat(draws, shape[position] // blocks).reshape([-1 if axis == position else 1 for axis in range(len(shape))])
    return level


def normal_values(own_key, dims, width, limit, cuts=(), held_as=jnp.bfloat16):
    result = jax.random.normal(own_key, dims, jnp.float32) * width
    if len(cuts) > 0:
        result = level_of(own_key, dims, cuts, -0.22, 0.18) * result
    return jnp.clip(result, min=-limit, max=limit).astype(held_as)


def setup_inputs(seed: int = 0) -> dict:
    key_list = jax.random.split(jax.random.key(seed), 7)
    e_field = normal_values(key_list[0], (3, NZ, NX, NY), 1.0, 6.0, ((2, 4), (3, 8)), jnp.float32)
    h_field = normal_values(key_list[1], (3, NZ, NX, NY), 1.0, 6.0, ((2, 4), (3, 8)), jnp.float32)
    e_coef = jnp.clip(jnp.exp(math.log(0.5) - 1.3862944 * jax.random.uniform(key_list[2], (NZ, NX, NY), jnp.float32) ** level_of(key_list[2], (NZ, NX, NY), ((1, 4), (2, 8)), -0.2, 0.2)), 0.125, 0.5)
    basis = normal_values(key_list[3], (RANK, NX, NY), (NX * NY) ** -0.5, 0.03125, ((0, 4), (2, 8)), jnp.float32)
    pml_width = place_ends(jax.random.randint(key_list[4], (4,), 2, 9), jax.random.fold_in(key_list[4], 1), 2, 8).astype(jnp.int32)
    snap_index = place_ends(jax.random.randint(key_list[5], (SNAPS,), 0, 6 * NZ), jax.random.fold_in(key_list[5], 1), 0, (6 * NZ) - 1).astype(jnp.int32)
    return {"e_field": e_field, "h_field": h_field, "e_coef": e_coef, "basis": basis, "pml_width": pml_width, "snap_index": snap_index}


time_step = 0.5
sigma_top = 4.0
alpha_shift = 0.05


def forward(field, axis, plane):
    count = field.shape[axis]
    after = jnp.concatenate([lax.slice_in_dim(field, 1, count, axis=axis), jnp.expand_dims(plane, axis)], axis)
    return after - field


def backward(field, axis, plane):
    count = field.shape[axis]
    before = jnp.concatenate([jnp.expand_dims(plane, axis), lax.slice_in_dim(field, 0, count - 1, axis=axis)], axis)
    return field - before


def absorber(positions, total, low, high):
    depth = jnp.maximum(jnp.maximum((low - positions) / low, (positions - (total - 1.0 - high)) / high), 0.0)
    sigma = sigma_top * depth ** 3
    damp = jnp.exp(-(sigma + alpha_shift) * time_step)
    gain = sigma / (sigma + alpha_shift) * (damp - 1.0)
    return damp, gain


def magnetic(e_field, h_field, psi, next_x, next_y, damp_x, gain_x, damp_y, gain_y):
    e_x, e_y, e_z = e_field[0], e_field[1], e_field[2]
    h_x, h_y, h_z = h_field[0], h_field[1], h_field[2]
    zplane = jnp.zeros_like(e_x[0])
    ez_dy = forward(e_z, 2, next_y[1])
    ey_dz = forward(e_y, 0, zplane)
    ex_dz = forward(e_x, 0, zplane)
    ez_dx = forward(e_z, 1, next_x[1])
    ey_dx = forward(e_y, 1, next_x[0])
    ex_dy = forward(e_x, 2, next_y[0])
    psi_hxy = damp_y * psi[0] + gain_y * ez_dy
    psi_hyx = damp_x * psi[1] + gain_x * ez_dx
    psi_hzx = damp_x * psi[2] + gain_x * ey_dx
    psi_hzy = damp_y * psi[3] + gain_y * ex_dy
    h_x = h_x - time_step * (ez_dy + psi_hxy - ey_dz)
    h_y = h_y - time_step * (ex_dz - ez_dx - psi_hyx)
    h_z = h_z - time_step * (ey_dx + psi_hzx - ex_dy - psi_hzy)
    return jnp.stack((h_x, h_y, h_z)), (psi_hxy, psi_hyx, psi_hzx, psi_hzy)


def electric(e_field, h_field, psi, e_coef, prev_x, prev_y, damp_x, gain_x, damp_y, gain_y):
    e_x, e_y, e_z = e_field[0], e_field[1], e_field[2]
    h_x, h_y, h_z = h_field[0], h_field[1], h_field[2]
    zplane = jnp.zeros_like(h_x[0])
    hz_dy = backward(h_z, 2, prev_y[1])
    hy_dz = backward(h_y, 0, zplane)
    hx_dz = backward(h_x, 0, zplane)
    hz_dx = backward(h_z, 1, prev_x[1])
    hy_dx = backward(h_y, 1, prev_x[0])
    hx_dy = backward(h_x, 2, prev_y[0])
    psi_exy = damp_y * psi[0] + gain_y * hz_dy
    psi_eyx = damp_x * psi[1] + gain_x * hz_dx
    psi_ezx = damp_x * psi[2] + gain_x * hy_dx
    psi_ezy = damp_y * psi[3] + gain_y * hx_dy
    e_x = e_x + e_coef * (hz_dy + psi_exy - hy_dz)
    e_y = e_y + e_coef * (hx_dz - hz_dx - psi_eyx)
    e_z = e_z + e_coef * (hy_dx + psi_ezx - hx_dy - psi_ezy)
    return jnp.stack((e_x, e_y, e_z)), (psi_exy, psi_eyx, psi_ezx, psi_ezy)


def reference(e_field, h_field, e_coef, basis, pml_width, snap_index):
    widths = pml_width.astype(jnp.float32)
    x_pos = jnp.arange(NX, dtype=jnp.float32)
    y_pos = jnp.arange(NY, dtype=jnp.float32)
    hdx, hgx = absorber(x_pos + 0.5, float(NX), widths[0], widths[1])
    hdy, hgy = absorber(y_pos + 0.5, float(NY), widths[2], widths[3])
    edx, egx = absorber(x_pos, float(NX), widths[0], widths[1])
    edy, egy = absorber(y_pos, float(NY), widths[2], widths[3])
    hdx, hgx, edx, egx = [v.reshape(1, NX, 1) for v in (hdx, hgx, edx, egx)]
    hdy, hgy, edy, egy = [v.reshape(1, 1, NY) for v in (hdy, hgy, edy, egy)]
    zeros_cells = jnp.zeros((NZ, NX, NY), jnp.float32)
    psi_mag = (zeros_cells,) * 4
    psi_ele = (zeros_cells,) * 4
    plane_x = jnp.zeros((2, NZ, NY), jnp.float32)
    plane_y = jnp.zeros((2, NZ, NX), jnp.float32)
    for step in range(STEPS):
        h_field, psi_mag = magnetic(e_field, h_field, psi_mag, plane_x, plane_y, hdx, hgx, hdy, hgy)
        e_field, psi_ele = electric(e_field, h_field, psi_ele, e_coef, plane_x, plane_y, edx, egx, edy, egy)
    planes = jnp.concatenate((e_field, h_field), 0).reshape(6 * NZ, NX, NY)
    snaps = jnp.take(planes, snap_index, axis=0).reshape(SNAPS, NX * NY)
    coefficients = jnp.dot(snaps, basis.reshape(RANK, NX * NY).T, precision=lax.Precision.HIGHEST)
    gram = jnp.dot(snaps, snaps.T, precision=lax.Precision.HIGHEST) / float(NX * NY)
    return e_field, h_field, coefficients, gram
```

```python
import functools
import jax
import jax.numpy as jnp
from jax import lax
from jax.experimental import pallas as pl
from jax.experimental.pallas import tpu as pltpu
from jax.sharding import PartitionSpec as P

STEPS = 8

time_step = 0.5
sigma_top = 4.0
alpha_shift = 0.05


def absorber(positions, total, low, high):
    depth = jnp.maximum(
        jnp.maximum((low - positions) / low, (positions - (total - 1.0 - high)) / high), 0.0
    )
    sigma = sigma_top * (depth * depth * depth)
    damp = jnp.exp(-(sigma + alpha_shift) * time_step)
    gain = sigma / (sigma + alpha_shift) * (damp - 1.0)
    return damp, gain


def step_kernel(
    n_row, n_col, width_ref, index_ref, e_in, h_in, coef_in, basis_in, e_out, h_out, proj_out, gram_out,
    fields, coef_s, psi, side_e, side_h, side_coef, side_psi, first_y, y_out, y_in,
    up_out, up_in, down_out, down_in, last_x, row_psi, before, before_psi, before_h,
    prof, modes, snaps, part, row_sums, col_sums, total,
    local_sem, y_send, y_recv, x_send, x_recv, mode_send, mode_recv,
    sum_send, sum_recv, col_send, col_recv, back_send, back_recv,
):
    e_s, h_s = fields.at[pl.ds(0, 3)], fields.at[pl.ds(3, 3)]
    nz, nx, ny = coef_s.shape
    width = STEPS
    group = ny // width
    size = group // 2
    chunks = nz // size
    half = ny // 2
    row, col = lax.axis_index("row"), lax.axis_index("col")
    up, down = row > 0, row < n_row - 1
    left, right = col > 0, col < n_col - 1

    load_e = pltpu.make_async_copy(e_in, e_s.at[:, pl.ds(0, nz)], local_sem.at[0])
    load_h = pltpu.make_async_copy(h_in, h_s.at[:, pl.ds(1, nz)], local_sem.at[1])
    load_c = pltpu.make_async_copy(coef_in, coef_s, local_sem.at[2])
    load_e.start()
    load_h.start()
    load_c.start()
    n_modes = basis_in.shape[0]
    modes_3d = modes.reshape(n_modes * n_row, nx, ny)
    load_b = pltpu.make_async_copy(
        basis_in.at[:, pl.ds(pl.multiple_of(row * nx, nx), nx)],
        modes_3d.at[pl.ds(row * n_modes, n_modes)], local_sem.at[3])
    load_b.start()
    row_peers = [lax.rem(row + k, n_row) for k in range(1, n_row)]
    col_peers = [lax.rem(col + k, n_col) for k in range(1, n_col)]

    part[...] = jnp.zeros_like(part)
    up_in[...] = jnp.zeros_like(up_in)
    down_in[...] = jnp.zeros_like(down_in)
    for side, there in enumerate((left, right)):
        @pl.when(jnp.logical_not(there))
        def _():
            y_in[side] = jnp.zeros(y_in.shape[1:], jnp.float32)

    barrier = pltpu.get_barrier_semaphore()
    for peer in row_peers:
        pl.semaphore_signal(
            barrier, inc=1, device_id={"row": peer, "col": col}, device_id_type=pl.DeviceIdType.MESH)
    for peer in col_peers:
        pl.semaphore_signal(
            barrier, inc=1, device_id={"row": row, "col": peer}, device_id_type=pl.DeviceIdType.MESH)

    zero = jnp.zeros((nx, ny), jnp.float32)
    for c in range(3):
        e_s[c, nz] = zero
        h_s[c, 0] = zero
        side_e[c, chunks] = zero
        side_h[c, 0] = zero
    last_x[0, chunks] = zero

    def clear(z, carry):
        for k in range(8):
            psi[k, z] = zero
        return carry

    lax.fori_loop(0, nz, clear, 0)
    side_psi[...] = jnp.zeros_like(side_psi)
    row_psi[...] = jnp.zeros_like(row_psi)
    before[...] = jnp.zeros_like(before)
    before_psi[...] = jnp.zeros_like(before_psi)

    sub = lax.broadcasted_iota(jnp.int32, (nx, ny), 0)
    lane = lax.broadcasted_iota(jnp.int32, (nx, ny), 1)
    spot = lax.rem(lane, width)
    block = lax.div(lax.rem(lane, half), width)
    on_left = lane < half
    w = [jnp.full((nx, ny), width_ref[k], jnp.int32).astype(jnp.float32) for k in range(4)]
    x_pos = (sub + row * nx).astype(jnp.float32)
    y_pos = (lane + col * ny).astype(jnp.float32)
    x_before = (jnp.zeros_like(sub) + (row * nx - 1)).astype(jnp.float32)
    x_last = (jnp.zeros_like(sub) + (row * nx + nx - 1)).astype(jnp.float32)
    y_side = (spot + col * ny + jnp.where(on_left, -width, ny)).astype(jnp.float32)
    full_x, full_y = float(nx * n_row), float(ny * n_col)
    pairs = (
        absorber(x_pos + 0.5, full_x, w[0], w[1]), absorber(y_pos + 0.5, full_y, w[2], w[3]),
        absorber(x_pos, full_x, w[0], w[1]), absorber(y_pos, full_y, w[2], w[3]),
        absorber(x_before + 0.5, full_x, w[0], w[1]), absorber(x_last + 0.5, full_x, w[0], w[1]),
        absorber(y_side + 0.5, full_y, w[2], w[3]), absorber(y_side, full_y, w[2], w[3]),
    )
    for k, (damp, gain) in enumerate(pairs):
        prof[2 * k] = damp
        prof[2 * k + 1] = gain
    side_step = time_step * jnp.where(on_left, left.astype(jnp.float32), right.astype(jnp.float32))
    up_mask = up.astype(jnp.float32)

    routes = ((up, {"row": row - 1, "col": col}), (down, {"row": row + 1, "col": col}))
    arrives = (down, up)
    rows = 2 * size + 2

    def copy_of(m, slot, k):
        src, dst = ((up_out, up_in), (down_out, down_in))[m]
        return pltpu.make_async_remote_copy(
            src_ref=src.at[k, pl.ds(0, rows)], dst_ref=dst.at[slot, k, pl.ds(0, rows)],
            send_sem=x_send.at[m, slot, k], recv_sem=x_recv.at[m, slot, k],
            device_id=routes[m][1], device_id_type=pl.DeviceIdType.MESH)

    def start(m, slot, k):
        @pl.when(routes[m][0])
        def _():
            copy_of(m, slot, k).start()

    def wait_recv(m, slot, k):
        @pl.when(arrives[m])
        def _():
            copy_of(m, slot, k).wait_recv()

    def wait_send(m, slot, k):
        @pl.when(routes[m][0])
        def _():
            copy_of(m, slot, k).wait_send()

    sides = ((left, {"row": row, "col": col - 1}), (right, {"row": row, "col": col + 1}))

    def y_copy(side):
        return pltpu.make_async_remote_copy(
            src_ref=y_out.at[side], dst_ref=y_in.at[1 - side], send_sem=y_send.at[side],
            recv_sem=y_recv.at[1 - side], device_id=sides[side][1], device_id_type=pl.DeviceIdType.MESH)

    def y_arrival(side):
        return pltpu.make_async_remote_copy(
            src_ref=y_out.at[1 - side], dst_ref=y_in.at[side], send_sem=y_send.at[1 - side],
            recv_sem=y_recv.at[side], device_id=sides[side][1], device_id_type=pl.DeviceIdType.MESH)

    load_e.wait()
    load_h.wait()
    load_c.wait()

    def plane(c, z):
        return e_s[c, z] if c < 3 else h_s[c - 3, z + 1] if c < 6 else coef_s[z]

    def pack_sides(q, carry):
        for c in range(7):
            first, last = zero, zero
            for i in range(group):
                value = plane(c, q * group + i)
                here = lax.div(lane, width) == i
                first = jnp.where(here, pltpu.roll(value, i * width, 1) if i else value, first)
                last = jnp.where(here, pltpu.roll(value, (i * width + width) % ny, 1) if (i + 1) % group else value, last)
            y_out[0, c, q] = first
            y_out[1, c, q] = last
        return carry

    lax.fori_loop(0, nz // group, pack_sides, 0)
    pl.semaphore_wait(barrier, n_row - 1 + n_col - 1)
    for side in range(2):
        @pl.when(sides[side][0])
        def _():
            y_copy(side).start()

    def first_pack(k, carry):
        fx, fz = zero, zero
        for j in range(size):
            z = k * size + j
            ex, ey, ez = e_s[0, z], e_s[1, z], e_s[2, z]
            hy, hz = h_s[1, z + 1], h_s[2, z + 1]
            up_out[k, j:j + 1, :] = ey[0:1]
            up_out[k, size + j:size + j + 1, :] = ez[0:1]
            down_out[k, j:j + 1, :] = hy[nx - 1:nx]
            down_out[k, size + j:size + j + 1, :] = hz[nx - 1:nx]
            for c, value in enumerate((ex, ey, ez)):
                last_x[c, k, j:j + 1, :] = value[nx - 1:nx]
            at = lane == j * width + width - 1
            fx = jnp.where(at, pltpu.roll(ex, j * width + width - 1, 1), fx)
            fz = jnp.where(at, pltpu.roll(ez, j * width + width - 1, 1), fz)
        first_y[0, k] = fx
        first_y[1, k] = fz
        return carry

    lax.fori_loop(0, chunks, first_pack, 0)

    for side in range(2):
        @pl.when(sides[side][0])
        def _():
            y_arrival(side).wait_recv()

    def unpack(q, carry):
        for c in range(7):
            a, b = y_in[0, c, q], y_in[1, c, q]
            values = jnp.where(on_left, a, pltpu.roll(b, half, 1)), jnp.where(on_left, pltpu.roll(a, half, 1), b)
            for i in range(2):
                if c < 3:
                    side_e[c, 2 * q + i] = values[i]
                elif c < 6:
                    side_h[c - 3, 2 * q + i + 1] = values[i]
                else:
                    side_coef[2 * q + i] = values[i]
        return carry

    lax.fori_loop(0, nz // group, unpack, 0)

    def z_after(here, after):
        return jnp.where(block == size - 1, pltpu.roll(after, half - width, 1), pltpu.roll(here, ny - width, 1))

    def z_before(here, prior):
        return jnp.where(block == 0, pltpu.roll(prior, half + width, 1), pltpu.roll(here, width, 1))

    def y_after(here, edge):
        return jnp.where(spot == width - 1, edge, pltpu.roll(here, ny - 1, 1))

    def y_before(here, edge):
        return jnp.where(spot == 0, edge, pltpu.roll(here, 1, 1))

    def spread(value):
        return jnp.broadcast_to(value, (nx, ny))

    def below(k):
        ex, ey, ez = last_x[0, k], last_x[1, k], last_x[2, k]
        hdy, hgy, ldx, lgx = prof[2], prof[3], prof[10], prof[11]
        ex_dz = jnp.where(sub == nx - 1, spread(last_x[0, k + 1, 0:1, :]), pltpu.roll(ex, nx - 1, 0)) - ex
        corner = jnp.where(lane == half + width * sub, spread(side_e[0, k, nx - 1:nx, :]), 0.0)
        corner = jnp.sum(corner, axis=1, keepdims=True)
        ex_dy = jnp.where(lane == ny - 1, corner, pltpu.roll(ex, ny - 1, 1)) - ex
        p1 = ldx * row_psi[0, k] - lgx * ez
        p2 = ldx * row_psi[1, k] - lgx * ey
        p3 = hdy * row_psi[2, k] + hgy * ex_dy
        row_psi[0, k], row_psi[1, k], row_psi[2, k] = p1, p2, p3
        down_out[k, 0:size, :] = down_out[k, 0:size, :] - time_step * (ex_dz + ez - p1)
        down_out[k, size:2 * size, :] = down_out[k, size:2 * size, :] - time_step * (p2 - ey - ex_dy - p3)
        ex, ey, ez = side_e[0, k], side_e[1, k], side_e[2, k]
        hdx, hgx, hdy, hgy = prof[0], prof[1], prof[12], prof[13]
        ex_dz = z_after(ex, side_e[0, k + 1]) - ex
        ex_dy = y_after(ex, first_y[0, k]) - ex
        p1 = hdx * side_psi[1, k] - hgx * ez
        p2 = hdx * side_psi[2, k] - hgx * ey
        p3 = hdy * side_psi[3, k] + hgy * ex_dy
        hy = side_h[1, k + 1] - side_step * (ex_dz + ez - p1)
        hz = side_h[2, k + 1] - side_step * (p2 - ey - ex_dy - p3)
        down_out[k, 2 * size:2 * size + 1, :] = hy[nx - 1:nx]
        down_out[k, 2 * size + 1:2 * size + 2, :] = hz[nx - 1:nx]

    def first_send(k, carry):
        up_out[k, 2 * size:2 * size + 1, :] = side_e[1, k, 0:1, :]
        up_out[k, 2 * size + 1:2 * size + 2, :] = side_e[2, k, 0:1, :]
        start(0, 0, k)
        below(k)
        start(1, 0, k)
        return carry

    lax.fori_loop(0, chunks, first_send, 0)
    piece = n_modes // STEPS

    def mode_copies(s):
        return [
            pltpu.make_async_remote_copy(
                src_ref=basis_in.at[pl.ds(s * piece, piece), pl.ds(pl.multiple_of(peer * nx, nx), nx)],
                dst_ref=modes_3d.at[pl.ds(row * n_modes + s * piece, piece)],
                send_sem=mode_send.at[k, s], recv_sem=mode_recv.at[k, s],
                device_id={"row": peer, "col": col}, device_id_type=pl.DeviceIdType.MESH)
            for k, peer in enumerate(row_peers)
        ]

    def tick(s, slot, k):
        more = s < STEPS - 1
        hdx, hgx, hdy, hgy = prof[0], prof[1], prof[2], prof[3]
        edx, egx, edy, egy = prof[4], prof[5], prof[6], prof[7]
        bdx, bgx = prof[8], prof[9]
        sdy, sgy = prof[12], prof[13]
        wait_recv(0, slot, k)
        ex, ey, ez = side_e[0, k], side_e[1, k], side_e[2, k]
        edge_ex, edge_ez = ex, ez
        row_y = spread(up_in[slot, k, 2 * size:2 * size + 1, :])
        row_z = spread(up_in[slot, k, 2 * size + 1:2 * size + 2, :])
        ey_dz = z_after(ey, side_e[1, k + 1]) - ey
        ex_dz = z_after(ex, side_e[0, k + 1]) - ex
        ez_dy = y_after(ez, first_y[1, k]) - ez
        ex_dy = y_after(ex, first_y[0, k]) - ex
        ez_dx = jnp.where(sub == nx - 1, row_z, pltpu.roll(ez, nx - 1, 0)) - ez
        ey_dx = jnp.where(sub == nx - 1, row_y, pltpu.roll(ey, nx - 1, 0)) - ey
        p0 = sdy * side_psi[0, k] + sgy * ez_dy
        p1 = hdx * side_psi[1, k] + hgx * ez_dx
        p2 = hdx * side_psi[2, k] + hgx * ey_dx
        p3 = sdy * side_psi[3, k] + sgy * ex_dy
        side_psi[0, k], side_psi[1, k], side_psi[2, k], side_psi[3, k] = p0, p1, p2, p3
        side_hx = side_h[0, k + 1] - side_step * (ez_dy + p0 - ey_dz)
        side_hy = side_h[1, k + 1] - side_step * (ex_dz - ez_dx - p1)
        side_hz = side_h[2, k + 1] - side_step * (ey_dx + p2 - ex_dy - p3)
        side_h[0, k + 1], side_h[1, k + 1], side_h[2, k + 1] = side_hx, side_hy, side_hz

        ey, ez = up_out[k, 0:size, :], up_out[k, size:2 * size, :]
        p1 = bdx * before_psi[0, k] + bgx * ez
        p2 = bdx * before_psi[1, k] + bgx * ey
        before_psi[0, k], before_psi[1, k] = p1, p2
        hy = before[0, k] + time_step * (ez + p1)
        hz = before[1, k] - time_step * (ey + p2)
        before[0, k], before[1, k] = hy, hz
        ey, ez = up_out[k, 2 * size:2 * size + 1, :], up_out[k, 2 * size + 1:2 * size + 2, :]
        factor = side_step[0:1] * (1.0 + bgx[0:1])
        wait_recv(1, slot, k)
        before_h[0:size, :] = up_mask * (hy + down_in[slot, k, 0:size, :])
        before_h[size:2 * size, :] = up_mask * (hz + down_in[slot, k, size:2 * size, :])
        back_y = up_mask * (down_in[slot, k, 2 * size:2 * size + 1, :] + factor * ez)
        back_z = up_mask * (down_in[slot, k, 2 * size + 1:2 * size + 2, :] - factor * ey)

        wait_send(0, slot, k)

        last_hx, last_hz, first_ex, first_ez = zero, zero, zero, zero
        below_hx, below_hy = h_s[0, k * size], h_s[1, k * size]
        ex, ey, ez = e_s[0, k * size], e_s[1, k * size], e_s[2, k * size]
        for j in range(size):
            z = k * size + j
            next_ex, next_ey, next_ez = e_s[0, z + 1], e_s[1, z + 1], e_s[2, z + 1]
            row_y = spread(up_in[slot, k, j:j + 1, :])
            row_z = spread(up_in[slot, k, size + j:size + j + 1, :])
            to_end = (ny - 1 - half - width * j) % ny
            col_x = pltpu.roll(edge_ex, to_end, 1)
            col_z = pltpu.roll(edge_ez, to_end, 1)
            ey_dz = next_ey - ey
            ex_dz = next_ex - ex
            ez_dy = jnp.where(lane == ny - 1, col_z, pltpu.roll(ez, ny - 1, 1)) - ez
            ex_dy = jnp.where(lane == ny - 1, col_x, pltpu.roll(ex, ny - 1, 1)) - ex
            ez_dx = jnp.where(sub == nx - 1, row_z, pltpu.roll(ez, nx - 1, 0)) - ez
            ey_dx = jnp.where(sub == nx - 1, row_y, pltpu.roll(ey, nx - 1, 0)) - ey
            p0 = hdy * psi[0, z] + hgy * ez_dy
            p1 = hdx * psi[1, z] + hgx * ez_dx
            p2 = hdx * psi[2, z] + hgx * ey_dx
            p3 = hdy * psi[3, z] + hgy * ex_dy
            psi[0, z], psi[1, z], psi[2, z], psi[3, z] = p0, p1, p2, p3
            hx = h_s[0, z + 1] - time_step * (ez_dy + p0 - ey_dz)
            hy = h_s[1, z + 1] - time_step * (ex_dz - ez_dx - p1)
            hz = h_s[2, z + 1] - time_step * (ey_dx + p2 - ex_dy - p3)
            h_s[0, z + 1], h_s[1, z + 1], h_s[2, z + 1] = hx, hy, hz
            at = lane == half + width * j
            last_hx = jnp.where(at, pltpu.roll(hx, (half + width * j + 1) % ny, 1), last_hx)
            last_hz = jnp.where(at, pltpu.roll(hz, (half + width * j + 1) % ny, 1), last_hz)

            row_y = spread(before_h[j:j + 1, :])
            row_z = spread(before_h[size + j:size + j + 1, :])
            to_start = ny - (width * j + width - 1)
            col_x = pltpu.roll(side_hx, to_start, 1)
            col_z = pltpu.roll(side_hz, to_start, 1)
            hy_dz = hy - below_hy
            hx_dz = hx - below_hx
            hz_dy = hz - jnp.where(lane == 0, col_z, pltpu.roll(hz, 1, 1))
            hx_dy = hx - jnp.where(lane == 0, col_x, pltpu.roll(hx, 1, 1))
            hz_dx = hz - jnp.where(sub == 0, row_z, pltpu.roll(hz, 1, 0))
            hy_dx = hy - jnp.where(sub == 0, row_y, pltpu.roll(hy, 1, 0))
            p0 = edy * psi[4, z] + egy * hz_dy
            p1 = edx * psi[5, z] + egx * hz_dx
            p2 = edx * psi[6, z] + egx * hy_dx
            p3 = edy * psi[7, z] + egy * hx_dy
            psi[4, z], psi[5, z], psi[6, z], psi[7, z] = p0, p1, p2, p3
            amount = coef_s[z]
            ex = ex + amount * (hz_dy + p0 - hy_dz)
            ey = ey + amount * (hx_dz - hz_dx - p1)
            ez = ez + amount * (hy_dx + p2 - hx_dy - p3)
            e_s[0, z], e_s[1, z], e_s[2, z] = ex, ey, ez
            at = lane == width * j + width - 1
            first_ex = jnp.where(at, pltpu.roll(ex, width * j + width - 1, 1), first_ex)
            first_ez = jnp.where(at, pltpu.roll(ez, width * j + width - 1, 1), first_ez)
            up_out[k, j:j + 1, :] = ey[0:1]
            up_out[k, size + j:size + j + 1, :] = ez[0:1]
            for c, value in enumerate((ex, ey, ez)):
                last_x[c, k, j:j + 1, :] = value[nx - 1:nx]
            below_hx, below_hy = hx, hy
            ex, ey, ez = next_ex, next_ey, next_ez
        first_y[0, k] = first_ex
        first_y[1, k] = first_ez

        sdy, sgy = prof[14], prof[15]
        hx, hy, hz = side_hx, side_hy, side_hz
        hy_dz = hy - z_before(hy, side_h[1, k])
        hx_dz = hx - z_before(hx, side_h[0, k])
        hz_dy = hz - y_before(hz, last_hz)
        hx_dy = hx - y_before(hx, last_hx)
        hz_dx = hz - jnp.where(sub == 0, spread(back_z), pltpu.roll(hz, 1, 0))
        hy_dx = hy - jnp.where(sub == 0, spread(back_y), pltpu.roll(hy, 1, 0))
        p0 = sdy * side_psi[4, k] + sgy * hz_dy
        p1 = edx * side_psi[5, k] + egx * hz_dx
        p2 = edx * side_psi[6, k] + egx * hy_dx
        p3 = sdy * side_psi[7, k] + sgy * hx_dy
        side_psi[4, k], side_psi[5, k], side_psi[6, k], side_psi[7, k] = p0, p1, p2, p3
        amount = side_coef[k]
        ex = side_e[0, k] + amount * (hz_dy + p0 - hy_dz)
        ey = side_e[1, k] + amount * (hx_dz - hz_dx - p1)
        ez = side_e[2, k] + amount * (hy_dx + p2 - hx_dy - p3)
        side_e[0, k], side_e[1, k], side_e[2, k] = ex, ey, ez
        up_out[k, 2 * size:2 * size + 1, :] = ey[0:1]
        up_out[k, 2 * size + 1:2 * size + 2, :] = ez[0:1]

        @pl.when(more)
        def _():
            start(0, 1 - slot, k)

    def send_below(s, slot, k):
        wait_send(1, slot, k)

        @pl.when(s < STEPS - 1)
        def _():
            below(k)
            start(1, 1 - slot, k)

    def step(s, carry):
        slot = lax.rem(s, 2)
        for copy in mode_copies(s):
            copy.start()

        def body(k, carry):
            tick(s, slot, k)

            @pl.when(k > 0)
            def _():
                send_below(s, slot, k - 1)

            return carry

        lax.fori_loop(0, chunks, body, 0)
        send_below(s, slot, chunks - 1)
        return carry

    lax.fori_loop(0, STEPS, step, 0)
    for side in range(2):
        @pl.when(sides[side][0])
        def _():
            y_copy(side).wait_send()

    store_e = pltpu.make_async_copy(e_s.at[:, pl.ds(0, nz)], e_out, local_sem.at[0])
    store_h = pltpu.make_async_copy(h_s.at[:, pl.ds(1, nz)], h_out, local_sem.at[1])
    store_e.start()
    store_h.start()

    count = snaps.shape[0] // nx

    def pick(s, carry):
        planes = []
        for j in range(8):
            index = index_ref[s * 8 + j]
            c = index // nz
            planes.append(fields[c, index - c * nz + (c // 3)])
        for j in range(8):
            snaps[pl.ds(pl.multiple_of((s * 8 + j) * nx, nx), nx), :] = planes[j]
        return carry

    lax.fori_loop(0, count // 8, pick, 0)
    load_b.wait()

    def wait_modes(s, carry):
        for copy in mode_copies(s):
            copy.wait()
        return carry

    lax.fori_loop(0, STEPS, wait_modes, 0)
    n_all = modes.shape[0] // nx
    dims = (((1,), (1,)), ((), ()))
    proj, gram = None, None
    for x in range(nx):
        a = snaps[pl.ds(x, count, stride=nx), :]
        b = modes[pl.ds(x, n_all, stride=nx), :]
        p = lax.dot_general(a, b, dims, precision=lax.Precision.HIGHEST, preferred_element_type=jnp.float32)
        g = lax.dot_general(a, a, dims, precision=lax.Precision.HIGHEST, preferred_element_type=jnp.float32)
        proj, gram = (p, g) if x == 0 else (proj + p, gram + g)
    part[:, 0:n_all] = proj
    part[:, n_all:n_all + count] = gram / float(nx * n_row * ny * n_col)

    share = count // n_row
    own = pl.ds(pl.multiple_of(row * share, share), share)

    def exchange(peers, axis, src_of, dst, sends, recvs):
        result = []
        for k, peer in enumerate(peers):
            where = {"row": row, "col": col}
            where[axis] = peer
            result.append(pltpu.make_async_remote_copy(
                src_ref=src_of(peer), dst_ref=dst, send_sem=sends.at[k], recv_sem=recvs.at[k],
                device_id=where, device_id_type=pl.DeviceIdType.MESH))
        for copy in result:
            copy.start()
        for copy in result:
            copy.wait()

    row_sums[row] = part[own, :]
    exchange(
        row_peers, "row", lambda peer: part.at[pl.ds(pl.multiple_of(peer * share, share), share)],
        row_sums.at[row], sum_send, sum_recv)
    value = row_sums[0]
    for k in range(1, n_row):
        value = value + row_sums[k]
    col_sums[col] = value
    exchange(col_peers, "col", lambda peer: col_sums.at[col], col_sums.at[col], col_send, col_recv)
    value = col_sums[0]
    for k in range(1, n_col):
        value = value + col_sums[k]
    total[own, :] = value
    exchange(row_peers, "row", lambda peer: total.at[own], total.at[own], back_send, back_recv)
    proj_out[...] = total[:, 0:n_all]
    gram_out[...] = total[:, n_all:n_all + count]
    store_e.wait()
    store_h.wait()


def shards(e_field, h_field, e_coef, basis, pml_width, snap_index):
    nz, nx, ny = e_coef.shape
    n_row, n_col = lax.axis_size("row"), lax.axis_size("col")
    modes, count = basis.shape[0] * n_row, snap_index.shape[0]
    f32 = jnp.float32
    size = ny // STEPS // 2
    chunks = nz // size
    wide = modes + (count + 127) // 128 * 128
    any_space = pl.BlockSpec(memory_space=pl.ANY)
    smem, vmem = pl.BlockSpec(memory_space=pltpu.SMEM), pl.BlockSpec(memory_space=pltpu.VMEM)
    return pl.pallas_call(
        functools.partial(step_kernel, n_row, n_col),
        out_shape=[
            jax.ShapeDtypeStruct(e_field.shape, f32), jax.ShapeDtypeStruct(h_field.shape, f32),
            jax.ShapeDtypeStruct((count, modes), f32), jax.ShapeDtypeStruct((count, count), f32),
        ],
        in_specs=[smem, smem, any_space, any_space, any_space, any_space],
        out_specs=[any_space, any_space, vmem, vmem],
        scratch_shapes=[
            pltpu.VMEM((6, nz + 1, nx, ny), f32),
            pltpu.VMEM((nz, nx, ny), f32), pltpu.VMEM((8, nz, nx, ny), f32),
            pltpu.VMEM((3, chunks + 1, nx, ny), f32), pltpu.VMEM((3, chunks + 1, nx, ny), f32),
            pltpu.VMEM((chunks, nx, ny), f32), pltpu.VMEM((8, chunks, nx, ny), f32),
            pltpu.VMEM((2, chunks, nx, ny), f32),
            pltpu.VMEM((2, 7, chunks // 2, nx, ny), f32), pltpu.VMEM((2, 7, chunks // 2, nx, ny), f32),
            pltpu.VMEM((chunks, 3 * size, ny), f32), pltpu.VMEM((2, chunks, 3 * size, ny), f32),
            pltpu.VMEM((chunks, 3 * size, ny), f32), pltpu.VMEM((2, chunks, 3 * size, ny), f32),
            pltpu.VMEM((3, chunks + 1, size, ny), f32), pltpu.VMEM((3, chunks, size, ny), f32),
            pltpu.VMEM((2, chunks, size, ny), f32), pltpu.VMEM((2, chunks, size, ny), f32),
            pltpu.VMEM((2 * size, ny), f32),
            pltpu.VMEM((16, nx, ny), f32),
            pltpu.VMEM((modes * nx, ny), f32), pltpu.VMEM((count * nx, ny), f32),
            pltpu.VMEM((count, wide), f32), pltpu.VMEM((n_row, count // n_row, wide), f32),
            pltpu.VMEM((n_col, count // n_row, wide), f32), pltpu.VMEM((count, wide), f32),
            pltpu.SemaphoreType.DMA((4,)),
            pltpu.SemaphoreType.DMA((2,)), pltpu.SemaphoreType.DMA((2,)),
            pltpu.SemaphoreType.DMA((2, 2, chunks)), pltpu.SemaphoreType.DMA((2, 2, chunks)),
            pltpu.SemaphoreType.DMA((n_row - 1, STEPS)), pltpu.SemaphoreType.DMA((n_row - 1, STEPS)),
            pltpu.SemaphoreType.DMA((n_row - 1,)), pltpu.SemaphoreType.DMA((n_row - 1,)),
            pltpu.SemaphoreType.DMA((n_col - 1,)), pltpu.SemaphoreType.DMA((n_col - 1,)),
            pltpu.SemaphoreType.DMA((n_row - 1,)), pltpu.SemaphoreType.DMA((n_row - 1,)),
        ],
        compiler_params=pltpu.CompilerParams(
            collective_id=0, has_side_effects=True, vmem_limit_bytes=67_043_328
        ),
    )(pml_width, snap_index, e_field, h_field, e_coef, basis)


def solution(mesh):
    in_specs = (
        P(None, None, "row", "col"),
        P(None, None, "row", "col"),
        P(None, "row", "col"),
        P("row", None, "col"),
        P(),
        P(),
    )
    out_specs = (P(None, None, "row", "col"), P(None, None, "row", "col"), P(), P())
    return jax.shard_map(shards, mesh=mesh, in_specs=in_specs, out_specs=out_specs, check_vma=False)
```

```python
import functools
import jax
import jax.numpy as jnp
from jax import lax
from jax.experimental import pallas as pl
from jax.experimental.pallas import tpu as pltpu
from jax.sharding import PartitionSpec as P

STEPS = 8

time_step = 0.5
sigma_top = 4.0
alpha_shift = 0.05


def absorber(positions, total, low, high):
    depth = jnp.maximum(
        jnp.maximum((low - positions) / low, (positions - (total - 1.0 - high)) / high), 0.0
    )
    sigma = sigma_top * (depth * depth * depth)
    damp = jnp.exp(-(sigma + alpha_shift) * time_step)
    gain = sigma / (sigma + alpha_shift) * (damp - 1.0)
    return damp, gain


def step_kernel(
    n_row, n_col, width_ref, index_ref, e_in, h_in, coef_in, basis_in, e_s, h_s, total,
    coef_s, psi, side_e, side_h, side_coef, side_psi, first_y, y_out, y_in,
    up_out, up_in, down_out, down_in, last_x, row_psi, before, before_psi, before_h,
    prof, modes, snaps, part, row_sums, col_sums,
    local_sem, y_send, y_recv, x_send, x_recv, mode_send, mode_recv,
    sum_send, sum_recv, col_send, col_recv, back_send, back_recv,
):
    nz, nx, ny = coef_s.shape
    width = STEPS
    group = ny // width
    size = group // 2
    chunks = nz // size
    half = ny // 2
    row, col = lax.axis_index("row"), lax.axis_index("col")
    up, down = row > 0, row < n_row - 1
    left, right = col > 0, col < n_col - 1

    load_e = pltpu.make_async_copy(e_in, e_s.at[:, pl.ds(0, nz)], local_sem.at[0])
    load_h = pltpu.make_async_copy(h_in, h_s.at[:, pl.ds(1, nz)], local_sem.at[1])
    load_c = pltpu.make_async_copy(coef_in, coef_s, local_sem.at[2])
    load_e.start()
    load_h.start()
    load_c.start()
    n_modes = basis_in.shape[0]
    modes_3d = modes.reshape(n_modes * n_row, nx, ny)
    load_b = pltpu.make_async_copy(
        basis_in.at[:, pl.ds(pl.multiple_of(row * nx, nx), nx)],
        modes_3d.at[pl.ds(row * n_modes, n_modes)], local_sem.at[3])
    load_b.start()
    row_peers = [lax.rem(row + k, n_row) for k in range(1, n_row)]
    pair = lax.rem(col, 2)
    near = [
        {"row": lax.rem(row + k, n_row), "col": col - pair + lax.rem(pair + m, 2)}
        for k in range(n_row) for m in range(2) if k + m]
    far = [{"row": row, "col": lax.rem(col + 2 * k, n_col)} for k in range(1, n_col // 2)]
    other = col - 1 + 2 * pair
    beside = jnp.logical_and(other >= 0, other < n_col)
    part[...] = jnp.zeros_like(part)
    up_in[...] = jnp.zeros_like(up_in)
    down_in[...] = jnp.zeros_like(down_in)
    for side, there in enumerate((left, right)):
        @pl.when(jnp.logical_not(there))
        def _():
            y_in[side] = jnp.zeros(y_in.shape[1:], jnp.float32)

    barrier = pltpu.get_barrier_semaphore()
    for peer in near + far:
        pl.semaphore_signal(barrier, inc=1, device_id=peer, device_id_type=pl.DeviceIdType.MESH)

    @pl.when(beside)
    def _():
        pl.semaphore_signal(
            barrier, inc=1, device_id={"row": row, "col": other}, device_id_type=pl.DeviceIdType.MESH)

    zero = jnp.zeros((nx, ny), jnp.float32)
    for c in range(3):
        e_s[c, nz] = zero
        h_s[c, 0] = zero
        side_e[c, chunks] = zero
        side_h[c, 0] = zero
    last_x[0, chunks] = zero

    def clear(z, carry):
        for k in range(8):
            psi[k, z] = zero
        return carry

    lax.fori_loop(0, nz, clear, 0)
    side_psi[...] = jnp.zeros_like(side_psi)
    row_psi[...] = jnp.zeros_like(row_psi)
    before[...] = jnp.zeros_like(before)
    before_psi[...] = jnp.zeros_like(before_psi)

    sub = lax.broadcasted_iota(jnp.int32, (nx, ny), 0)
    lane = lax.broadcasted_iota(jnp.int32, (nx, ny), 1)
    spot = lax.rem(lane, width)
    block = lax.div(lax.rem(lane, half), width)
    on_left = lane < half
    w = [jnp.full((nx, ny), width_ref[k], jnp.int32).astype(jnp.float32) for k in range(4)]
    x_pos = (sub + row * nx).astype(jnp.float32)
    y_pos = (lane + col * ny).astype(jnp.float32)
    x_before = (jnp.zeros_like(sub) + (row * nx - 1)).astype(jnp.float32)
    x_last = (jnp.zeros_like(sub) + (row * nx + nx - 1)).astype(jnp.float32)
    y_side = (spot + col * ny + jnp.where(on_left, -width, ny)).astype(jnp.float32)
    full_x, full_y = float(nx * n_row), float(ny * n_col)
    pairs = (
        absorber(x_pos + 0.5, full_x, w[0], w[1]), absorber(y_pos + 0.5, full_y, w[2], w[3]),
        absorber(x_pos, full_x, w[0], w[1]), absorber(y_pos, full_y, w[2], w[3]),
        absorber(x_before + 0.5, full_x, w[0], w[1]), absorber(x_last + 0.5, full_x, w[0], w[1]),
        absorber(y_side + 0.5, full_y, w[2], w[3]), absorber(y_side, full_y, w[2], w[3]),
    )
    for k, (damp, gain) in enumerate(pairs):
        prof[2 * k] = damp
        prof[2 * k + 1] = gain
    side_step = time_step * jnp.where(on_left, left.astype(jnp.float32), right.astype(jnp.float32))
    up_mask = up.astype(jnp.float32)

    routes = ((up, {"row": row - 1, "col": col}), (down, {"row": row + 1, "col": col}))
    arrives = (down, up)
    rows = 2 * size + 2

    def copy_of(m, slot, k):
        src, dst = ((up_out, up_in), (down_out, down_in))[m]
        return pltpu.make_async_remote_copy(
            src_ref=src.at[k, pl.ds(0, rows)], dst_ref=dst.at[slot, k, pl.ds(0, rows)],
            send_sem=x_send.at[m, slot, k], recv_sem=x_recv.at[m, slot, k],
            device_id=routes[m][1], device_id_type=pl.DeviceIdType.MESH)

    def start(m, slot, k):
        @pl.when(routes[m][0])
        def _():
            copy_of(m, slot, k).start()

    def wait_recv(m, slot, k):
        @pl.when(arrives[m])
        def _():
            copy_of(m, slot, k).wait_recv()

    def wait_send(m, slot, k):
        @pl.when(routes[m][0])
        def _():
            copy_of(m, slot, k).wait_send()

    sides = ((left, {"row": row, "col": col - 1}), (right, {"row": row, "col": col + 1}))

    def y_copy(side):
        return pltpu.make_async_remote_copy(
            src_ref=y_out.at[side], dst_ref=y_in.at[1 - side], send_sem=y_send.at[side],
            recv_sem=y_recv.at[1 - side], device_id=sides[side][1], device_id_type=pl.DeviceIdType.MESH)

    def y_arrival(side):
        return pltpu.make_async_remote_copy(
            src_ref=y_out.at[1 - side], dst_ref=y_in.at[side], send_sem=y_send.at[1 - side],
            recv_sem=y_recv.at[side], device_id=sides[side][1], device_id_type=pl.DeviceIdType.MESH)

    load_e.wait()
    load_h.wait()
    load_c.wait()

    def plane(c, z):
        return e_s[c, z] if c < 3 else h_s[c - 3, z + 1] if c < 6 else coef_s[z]

    def pack_sides(q, carry):
        for c in range(7):
            first, last = zero, zero
            for i in range(group):
                value = plane(c, q * group + i)
                here = lax.div(lane, width) == i
                first = jnp.where(here, pltpu.roll(value, i * width, 1) if i else value, first)
                last = jnp.where(here, pltpu.roll(value, (i * width + width) % ny, 1) if (i + 1) % group else value, last)
            y_out[0, c, q] = first
            y_out[1, c, q] = last
        return carry

    lax.fori_loop(0, nz // group, pack_sides, 0)
    pl.semaphore_wait(barrier, len(near) + len(far) + beside.astype(jnp.int32))
    for side in range(2):
        @pl.when(sides[side][0])
        def _():
            y_copy(side).start()

    def first_pack(k, carry):
        fx, fz = zero, zero
        for j in range(size):
            z = k * size + j
            ex, ey, ez = e_s[0, z], e_s[1, z], e_s[2, z]
            hy, hz = h_s[1, z + 1], h_s[2, z + 1]
            up_out[k, j:j + 1, :] = ey[0:1]
            up_out[k, size + j:size + j + 1, :] = ez[0:1]
            down_out[k, j:j + 1, :] = hy[nx - 1:nx]
            down_out[k, size + j:size + j + 1, :] = hz[nx - 1:nx]
            for c, value in enumerate((ex, ey, ez)):
                last_x[c, k, j:j + 1, :] = value[nx - 1:nx]
            at = lane == j * width + width - 1
            fx = jnp.where(at, pltpu.roll(ex, j * width + width - 1, 1), fx)
            fz = jnp.where(at, pltpu.roll(ez, j * width + width - 1, 1), fz)
        first_y[0, k] = fx
        first_y[1, k] = fz
        return carry

    lax.fori_loop(0, chunks, first_pack, 0)

    for side in range(2):
        @pl.when(sides[side][0])
        def _():
            y_arrival(side).wait_recv()

    def unpack(q, carry):
        for c in range(7):
            a, b = y_in[0, c, q], y_in[1, c, q]
            values = jnp.where(on_left, a, pltpu.roll(b, half, 1)), jnp.where(on_left, pltpu.roll(a, half, 1), b)
            for i in range(2):
                if c < 3:
                    side_e[c, 2 * q + i] = values[i]
                elif c < 6:
                    side_h[c - 3, 2 * q + i + 1] = values[i]
                else:
                    side_coef[2 * q + i] = values[i]
        return carry

    lax.fori_loop(0, nz // group, unpack, 0)

    def z_after(here, after):
        return jnp.where(block == size - 1, pltpu.roll(after, half - width, 1), pltpu.roll(here, ny - width, 1))

    def z_before(here, prior):
        return jnp.where(block == 0, pltpu.roll(prior, half + width, 1), pltpu.roll(here, width, 1))

    def y_after(here, edge):
        return jnp.where(spot == width - 1, edge, pltpu.roll(here, ny - 1, 1))

    def y_before(here, edge):
        return jnp.where(spot == 0, edge, pltpu.roll(here, 1, 1))

    def spread(value):
        return jnp.broadcast_to(value, (nx, ny))

    def below(k):
        ex, ey, ez = last_x[0, k], last_x[1, k], last_x[2, k]
        hdy, hgy, ldx, lgx = prof[2], prof[3], prof[10], prof[11]
        ex_dz = jnp.where(sub == nx - 1, spread(last_x[0, k + 1, 0:1, :]), pltpu.roll(ex, nx - 1, 0)) - ex
        corner = jnp.where(lane == half + width * sub, spread(side_e[0, k, nx - 1:nx, :]), 0.0)
        corner = jnp.sum(corner, axis=1, keepdims=True)
        ex_dy = jnp.where(lane == ny - 1, corner, pltpu.roll(ex, ny - 1, 1)) - ex
        p1 = ldx * row_psi[0, k] - lgx * ez
        p2 = ldx * row_psi[1, k] - lgx * ey
        p3 = hdy * row_psi[2, k] + hgy * ex_dy
        row_psi[0, k], row_psi[1, k], row_psi[2, k] = p1, p2, p3
        down_out[k, 0:size, :] = down_out[k, 0:size, :] - time_step * (ex_dz + ez - p1)
        down_out[k, size:2 * size, :] = down_out[k, size:2 * size, :] - time_step * (p2 - ey - ex_dy - p3)
        ex, ey, ez = side_e[0, k], side_e[1, k], side_e[2, k]
        hdx, hgx, hdy, hgy = prof[0], prof[1], prof[12], prof[13]
        ex_dz = z_after(ex, side_e[0, k + 1]) - ex
        ex_dy = y_after(ex, first_y[0, k]) - ex
        p1 = hdx * side_psi[1, k] - hgx * ez
        p2 = hdx * side_psi[2, k] - hgx * ey
        p3 = hdy * side_psi[3, k] + hgy * ex_dy
        hy = side_h[1, k + 1] - side_step * (ex_dz + ez - p1)
        hz = side_h[2, k + 1] - side_step * (p2 - ey - ex_dy - p3)
        down_out[k, 2 * size:2 * size + 1, :] = hy[nx - 1:nx]
        down_out[k, 2 * size + 1:2 * size + 2, :] = hz[nx - 1:nx]

    def first_send(k, carry):
        up_out[k, 2 * size:2 * size + 1, :] = side_e[1, k, 0:1, :]
        up_out[k, 2 * size + 1:2 * size + 2, :] = side_e[2, k, 0:1, :]
        start(0, 0, k)
        below(k)
        start(1, 0, k)
        return carry

    lax.fori_loop(0, chunks, first_send, 0)
    piece = n_modes // STEPS

    def mode_copies(s):
        return [
            pltpu.make_async_remote_copy(
                src_ref=basis_in.at[pl.ds(s * piece, piece), pl.ds(pl.multiple_of(peer * nx, nx), nx)],
                dst_ref=modes_3d.at[pl.ds(row * n_modes + s * piece, piece)],
                send_sem=mode_send.at[k, s], recv_sem=mode_recv.at[k, s],
                device_id={"row": peer, "col": col}, device_id_type=pl.DeviceIdType.MESH)
            for k, peer in enumerate(row_peers)
        ]

    def tick(s, slot, k):
        more = s < STEPS - 1
        hdx, hgx, hdy, hgy = prof[0], prof[1], prof[2], prof[3]
        edx, egx, edy, egy = prof[4], prof[5], prof[6], prof[7]
        bdx, bgx = prof[8], prof[9]
        sdy, sgy = prof[12], prof[13]
        wait_recv(0, slot, k)
        ex, ey, ez = side_e[0, k], side_e[1, k], side_e[2, k]
        edge_ex, edge_ez = ex, ez
        row_y = spread(up_in[slot, k, 2 * size:2 * size + 1, :])
        row_z = spread(up_in[slot, k, 2 * size + 1:2 * size + 2, :])
        ey_dz = z_after(ey, side_e[1, k + 1]) - ey
        ex_dz = z_after(ex, side_e[0, k + 1]) - ex
        ez_dy = y_after(ez, first_y[1, k]) - ez
        ex_dy = y_after(ex, first_y[0, k]) - ex
        ez_dx = jnp.where(sub == nx - 1, row_z, pltpu.roll(ez, nx - 1, 0)) - ez
        ey_dx = jnp.where(sub == nx - 1, row_y, pltpu.roll(ey, nx - 1, 0)) - ey
        p0 = sdy * side_psi[0, k] + sgy * ez_dy
        p1 = hdx * side_psi[1, k] + hgx * ez_dx
        p2 = hdx * side_psi[2, k] + hgx * ey_dx
        p3 = sdy * side_psi[3, k] + sgy * ex_dy
        side_psi[0, k], side_psi[1, k], side_psi[2, k], side_psi[3, k] = p0, p1, p2, p3
        side_hx = side_h[0, k + 1] - side_step * (ez_dy + p0 - ey_dz)
        side_hy = side_h[1, k + 1] - side_step * (ex_dz - ez_dx - p1)
        side_hz = side_h[2, k + 1] - side_step * (ey_dx + p2 - ex_dy - p3)
        side_h[0, k + 1], side_h[1, k + 1], side_h[2, k + 1] = side_hx, side_hy, side_hz

        ey, ez = up_out[k, 0:size, :], up_out[k, size:2 * size, :]
        p1 = bdx * before_psi[0, k] + bgx * ez
        p2 = bdx * before_psi[1, k] + bgx * ey
        before_psi[0, k], before_psi[1, k] = p1, p2
        hy = before[0, k] + time_step * (ez + p1)
        hz = before[1, k] - time_step * (ey + p2)
        before[0, k], before[1, k] = hy, hz
        ey, ez = up_out[k, 2 * size:2 * size + 1, :], up_out[k, 2 * size + 1:2 * size + 2, :]
        factor = side_step[0:1] * (1.0 + bgx[0:1])
        wait_recv(1, slot, k)
        before_h[0:size, :] = up_mask * (hy + down_in[slot, k, 0:size, :])
        before_h[size:2 * size, :] = up_mask * (hz + down_in[slot, k, size:2 * size, :])
        back_y = up_mask * (down_in[slot, k, 2 * size:2 * size + 1, :] + factor * ez)
        back_z = up_mask * (down_in[slot, k, 2 * size + 1:2 * size + 2, :] - factor * ey)

        wait_send(0, slot, k)

        last_hx, last_hz, first_ex, first_ez = zero, zero, zero, zero
        below_hx, below_hy = h_s[0, k * size], h_s[1, k * size]
        ex, ey, ez = e_s[0, k * size], e_s[1, k * size], e_s[2, k * size]
        for j in range(size):
            z = k * size + j
            next_ex, next_ey, next_ez = e_s[0, z + 1], e_s[1, z + 1], e_s[2, z + 1]
            row_y = spread(up_in[slot, k, j:j + 1, :])
            row_z = spread(up_in[slot, k, size + j:size + j + 1, :])
            to_end = (ny - 1 - half - width * j) % ny
            col_x = pltpu.roll(edge_ex, to_end, 1)
            col_z = pltpu.roll(edge_ez, to_end, 1)
            ey_dz = next_ey - ey
            ex_dz = next_ex - ex
            ez_dy = jnp.where(lane == ny - 1, col_z, pltpu.roll(ez, ny - 1, 1)) - ez
            ex_dy = jnp.where(lane == ny - 1, col_x, pltpu.roll(ex, ny - 1, 1)) - ex
            ez_dx = jnp.where(sub == nx - 1, row_z, pltpu.roll(ez, nx - 1, 0)) - ez
            ey_dx = jnp.where(sub == nx - 1, row_y, pltpu.roll(ey, nx - 1, 0)) - ey
            p0 = hdy * psi[0, z] + hgy * ez_dy
            p1 = hdx * psi[1, z] + hgx * ez_dx
            p2 = hdx * psi[2, z] + hgx * ey_dx
            p3 = hdy * psi[3, z] + hgy * ex_dy
            psi[0, z], psi[1, z], psi[2, z], psi[3, z] = p0, p1, p2, p3
            hx = h_s[0, z + 1] - time_step * (ez_dy + p0 - ey_dz)
            hy = h_s[1, z + 1] - time_step * (ex_dz - ez_dx - p1)
            hz = h_s[2, z + 1] - time_step * (ey_dx + p2 - ex_dy - p3)
            h_s[0, z + 1], h_s[1, z + 1], h_s[2, z + 1] = hx, hy, hz
            at = lane == half + width * j
            last_hx = jnp.where(at, pltpu.roll(hx, (half + width * j + 1) % ny, 1), last_hx)
            last_hz = jnp.where(at, pltpu.roll(hz, (half + width * j + 1) % ny, 1), last_hz)

            row_y = spread(before_h[j:j + 1, :])
            row_z = spread(before_h[size + j:size + j + 1, :])
            to_start = ny - (width * j + width - 1)
            col_x = pltpu.roll(side_hx, to_start, 1)
            col_z = pltpu.roll(side_hz, to_start, 1)
            hy_dz = hy - below_hy
            hx_dz = hx - below_hx
            hz_dy = hz - jnp.where(lane == 0, col_z, pltpu.roll(hz, 1, 1))
            hx_dy = hx - jnp.where(lane == 0, col_x, pltpu.roll(hx, 1, 1))
            hz_dx = hz - jnp.where(sub == 0, row_z, pltpu.roll(hz, 1, 0))
            hy_dx = hy - jnp.where(sub == 0, row_y, pltpu.roll(hy, 1, 0))
            p0 = edy * psi[4, z] + egy * hz_dy
            p1 = edx * psi[5, z] + egx * hz_dx
            p2 = edx * psi[6, z] + egx * hy_dx
            p3 = edy * psi[7, z] + egy * hx_dy
            psi[4, z], psi[5, z], psi[6, z], psi[7, z] = p0, p1, p2, p3
            amount = coef_s[z]
            ex = ex + amount * (hz_dy + p0 - hy_dz)
            ey = ey + amount * (hx_dz - hz_dx - p1)
            ez = ez + amount * (hy_dx + p2 - hx_dy - p3)
            e_s[0, z], e_s[1, z], e_s[2, z] = ex, ey, ez
            at = lane == width * j + width - 1
            first_ex = jnp.where(at, pltpu.roll(ex, width * j + width - 1, 1), first_ex)
            first_ez = jnp.where(at, pltpu.roll(ez, width * j + width - 1, 1), first_ez)
            up_out[k, j:j + 1, :] = ey[0:1]
            up_out[k, size + j:size + j + 1, :] = ez[0:1]
            for c, value in enumerate((ex, ey, ez)):
                last_x[c, k, j:j + 1, :] = value[nx - 1:nx]
            below_hx, below_hy = hx, hy
            ex, ey, ez = next_ex, next_ey, next_ez
        first_y[0, k] = first_ex
        first_y[1, k] = first_ez

        sdy, sgy = prof[14], prof[15]
        hx, hy, hz = side_hx, side_hy, side_hz
        hy_dz = hy - z_before(hy, side_h[1, k])
        hx_dz = hx - z_before(hx, side_h[0, k])
        hz_dy = hz - y_before(hz, last_hz)
        hx_dy = hx - y_before(hx, last_hx)
        hz_dx = hz - jnp.where(sub == 0, spread(back_z), pltpu.roll(hz, 1, 0))
        hy_dx = hy - jnp.where(sub == 0, spread(back_y), pltpu.roll(hy, 1, 0))
        p0 = sdy * side_psi[4, k] + sgy * hz_dy
        p1 = edx * side_psi[5, k] + egx * hz_dx
        p2 = edx * side_psi[6, k] + egx * hy_dx
        p3 = sdy * side_psi[7, k] + sgy * hx_dy
        side_psi[4, k], side_psi[5, k], side_psi[6, k], side_psi[7, k] = p0, p1, p2, p3
        amount = side_coef[k]
        ex = side_e[0, k] + amount * (hz_dy + p0 - hy_dz)
        ey = side_e[1, k] + amount * (hx_dz - hz_dx - p1)
        ez = side_e[2, k] + amount * (hy_dx + p2 - hx_dy - p3)
        side_e[0, k], side_e[1, k], side_e[2, k] = ex, ey, ez
        up_out[k, 2 * size:2 * size + 1, :] = ey[0:1]
        up_out[k, 2 * size + 1:2 * size + 2, :] = ez[0:1]

        @pl.when(more)
        def _():
            start(0, 1 - slot, k)

    def send_below(s, slot, k):
        wait_send(1, slot, k)

        @pl.when(s < STEPS - 1)
        def _():
            below(k)
            start(1, 1 - slot, k)

    def step(s, carry):
        slot = lax.rem(s, 2)
        for copy in mode_copies(s):
            copy.start()

        def body(k, carry):
            tick(s, slot, k)

            @pl.when(k > 0)
            def _():
                send_below(s, slot, k - 1)

            return carry

        lax.fori_loop(0, chunks, body, 0)
        send_below(s, slot, chunks - 1)
        return carry

    lax.fori_loop(0, STEPS, step, 0)
    for side in range(2):
        @pl.when(sides[side][0])
        def _():
            y_copy(side).wait_send()

    count = snaps.shape[0] // nx

    def pick(s, carry):
        planes = []
        for j in range(8):
            index = index_ref[s * 8 + j]
            c = index // nz
            z = index - c * nz
            e_plane = e_s[jnp.minimum(c, 2), z]
            h_plane = h_s[jnp.maximum(c - 3, 0), z + 1]
            planes.append(jnp.where(c < 3, e_plane, h_plane))
        for j in range(8):
            snaps[pl.ds(pl.multiple_of((s * 8 + j) * nx, nx), nx), :] = planes[j]
        return carry

    lax.fori_loop(0, count // 8, pick, 0)
    load_b.wait()

    def wait_modes(s, carry):
        for copy in mode_copies(s):
            copy.wait()
        return carry

    lax.fori_loop(0, STEPS, wait_modes, 0)
    n_all = modes.shape[0] // nx
    dims = (((1,), (1,)), ((), ()))
    proj, gram = None, None
    for x in range(nx):
        a = snaps[pl.ds(x, count, stride=nx), :]
        b = modes[pl.ds(x, n_all, stride=nx), :]
        p = lax.dot_general(a, b, dims, precision=lax.Precision.HIGHEST, preferred_element_type=jnp.float32)
        g = lax.dot_general(a, a, dims, precision=lax.Precision.HIGHEST, preferred_element_type=jnp.float32)
        proj, gram = (p, g) if x == 0 else (proj + p, gram + g)
    gram = gram / float(nx * n_row * ny * n_col)
    share = part.shape[1]
    for k in range(part.shape[0]):
        part[k, :, 0:n_all] = proj[k * share:(k + 1) * share]
        part[k, :, n_all:n_all + count] = gram[k * share:(k + 1) * share]
    own = 2 * row + pair

    def exchange(peers, src_of, dst, sends, recvs):
        result = []
        for k, peer in enumerate(peers):
            result.append(pltpu.make_async_remote_copy(
                src_ref=src_of(peer), dst_ref=dst, send_sem=sends.at[k], recv_sem=recvs.at[k],
                device_id=peer, device_id_type=pl.DeviceIdType.MESH))
        for copy in result:
            copy.start()
        for copy in result:
            copy.wait()

    row_sums[own] = part[own]
    exchange(
        near, lambda peer: part.at[2 * peer["row"] + lax.rem(peer["col"], 2)],
        row_sums.at[own], sum_send, sum_recv)
    value = row_sums[0]
    for k in range(1, 2 * n_row):
        value = value + row_sums[k]
    level = lax.div(col, 2)
    col_sums[level] = value
    exchange(far, lambda peer: col_sums.at[level], col_sums.at[level], col_send, col_recv)
    value = col_sums[0]
    for k in range(1, n_col // 2):
        value = value + col_sums[k]
    total[own] = value
    exchange(near, lambda peer: total.at[own], total.at[own], back_send, back_recv)


def write_kernel(e_s, h_s, total, e_out, h_out, proj_out, gram_out, sems):
    nz = e_out.shape[1]
    store_e = pltpu.make_async_copy(e_s.at[:, pl.ds(0, nz)], e_out, sems.at[0])
    store_h = pltpu.make_async_copy(h_s.at[:, pl.ds(1, nz)], h_out, sems.at[1])
    store_e.start()
    store_h.start()
    n_all, count = proj_out.shape[1], gram_out.shape[1]
    share = total.shape[1]
    for k in range(total.shape[0]):
        proj_out[k * share:(k + 1) * share, :] = total[k, :, 0:n_all]
        gram_out[k * share:(k + 1) * share, :] = total[k, :, n_all:n_all + count]
    store_e.wait()
    store_h.wait()


def shards(e_field, h_field, e_coef, basis, pml_width, snap_index):
    nz, nx, ny = e_coef.shape
    n_row, n_col = lax.axis_size("row"), lax.axis_size("col")
    modes, count = basis.shape[0] * n_row, snap_index.shape[0]
    f32 = jnp.float32
    size = ny // STEPS // 2
    chunks = nz // size
    wide = modes + (count + 127) // 128 * 128
    any_space = pl.BlockSpec(memory_space=pltpu.HBM)
    smem, vmem = pl.BlockSpec(memory_space=pltpu.SMEM), pl.BlockSpec(memory_space=pltpu.VMEM)
    held = pltpu.VMEM((3, nz + 1, nx, ny), f32)
    share = count // (2 * n_row)
    e_s, h_s, total = pl.pallas_call(
        functools.partial(step_kernel, n_row, n_col),
        out_shape=[held, held, pltpu.VMEM((2 * n_row, share, wide), f32)],
        in_specs=[smem, smem, any_space, any_space, any_space, any_space],
        out_specs=[vmem, vmem, vmem],
        scratch_shapes=[
            pltpu.VMEM((nz, nx, ny), f32), pltpu.VMEM((8, nz, nx, ny), f32),
            pltpu.VMEM((3, chunks + 1, nx, ny), f32), pltpu.VMEM((3, chunks + 1, nx, ny), f32),
            pltpu.VMEM((chunks, nx, ny), f32), pltpu.VMEM((8, chunks, nx, ny), f32),
            pltpu.VMEM((2, chunks, nx, ny), f32),
            pltpu.VMEM((2, 7, chunks // 2, nx, ny), f32), pltpu.VMEM((2, 7, chunks // 2, nx, ny), f32),
            pltpu.VMEM((chunks, 3 * size, ny), f32), pltpu.VMEM((2, chunks, 3 * size, ny), f32),
            pltpu.VMEM((chunks, 3 * size, ny), f32), pltpu.VMEM((2, chunks, 3 * size, ny), f32),
            pltpu.VMEM((3, chunks + 1, size, ny), f32), pltpu.VMEM((3, chunks, size, ny), f32),
            pltpu.VMEM((2, chunks, size, ny), f32), pltpu.VMEM((2, chunks, size, ny), f32),
            pltpu.VMEM((2 * size, ny), f32),
            pltpu.VMEM((16, nx, ny), f32),
            pltpu.VMEM((modes * nx, ny), f32), pltpu.VMEM((count * nx, ny), f32),
            pltpu.VMEM((2 * n_row, share, wide), f32), pltpu.VMEM((2 * n_row, share, wide), f32),
            pltpu.VMEM((n_col // 2, share, wide), f32),
            pltpu.SemaphoreType.DMA((4,)),
            pltpu.SemaphoreType.DMA((2,)), pltpu.SemaphoreType.DMA((2,)),
            pltpu.SemaphoreType.DMA((2, 2, chunks)), pltpu.SemaphoreType.DMA((2, 2, chunks)),
            pltpu.SemaphoreType.DMA((n_row - 1, STEPS)), pltpu.SemaphoreType.DMA((n_row - 1, STEPS)),
            pltpu.SemaphoreType.DMA((2 * n_row - 1,)), pltpu.SemaphoreType.DMA((2 * n_row - 1,)),
            pltpu.SemaphoreType.DMA((n_col // 2 - 1,)), pltpu.SemaphoreType.DMA((n_col // 2 - 1,)),
            pltpu.SemaphoreType.DMA((2 * n_row - 1,)), pltpu.SemaphoreType.DMA((2 * n_row - 1,)),
        ],
        compiler_params=pltpu.CompilerParams(
            collective_id=0, has_side_effects=True, vmem_limit_bytes=65_280_000
        ),
    )(pml_width, snap_index, e_field, h_field, e_coef, basis)
    return pl.pallas_call(
        write_kernel,
        out_shape=[
            jax.ShapeDtypeStruct(e_field.shape, f32), jax.ShapeDtypeStruct(h_field.shape, f32),
            jax.ShapeDtypeStruct((count, modes), f32), jax.ShapeDtypeStruct((count, count), f32),
        ],
        in_specs=[vmem, vmem, vmem],
        out_specs=[any_space, any_space, vmem, vmem],
        scratch_shapes=[pltpu.SemaphoreType.DMA((2,))],
        compiler_params=pltpu.CompilerParams(vmem_limit_bytes=16_777_216),
    )(e_s, h_s, total)


def solution(mesh):
    in_specs = (
        P(None, None, "row", "col"),
        P(None, None, "row", "col"),
        P(None, "row", "col"),
        P("row", None, "col"),
        P(),
        P(),
    )
    out_specs = (P(None, None, "row", "col"), P(None, None, "row", "col"), P(), P())
    return jax.shard_map(shards, mesh=mesh, in_specs=in_specs, out_specs=out_specs, check_vma=False)
```

```python
import functools
import jax
import jax.numpy as jnp
from jax import lax
from jax.experimental import pallas as pl
from jax.experimental.pallas import tpu as pltpu
from jax.sharding import PartitionSpec as P

STEPS = 8


time_step = 0.5
sigma_top = 4.0
alpha_shift = 0.05


def absorber(positions, total, low, high):
    depth = jnp.maximum(
        jnp.maximum((low - positions) / low, (positions - (total - 1.0 - high)) / high), 0.0
    )
    sigma = sigma_top * (depth * depth * depth)
    damp = jnp.exp(-(sigma + alpha_shift) * time_step)
    gain = sigma / (sigma + alpha_shift) * (damp - 1.0)
    return damp, gain


def step_kernel(
    n_row, n_col, width_ref, index_ref, e_in, h_in, coef_in, basis_in, e_s, h_s, total,
    coef_s, psi, side_e, side_h, side_coef, side_psi, first_y, y_out, y_in,
    up_out, up_in, down_out, down_in, last_x, row_psi, before, before_psi, before_h,
    prof, modes, snaps, part, row_sums, col_sums,
    local_sem, y_send, y_recv, x_send, x_recv, mode_send, mode_recv,
    sum_send, sum_recv, col_send, col_recv, back_send, back_recv,
):
    nz, nx, ny = coef_s.shape
    width = STEPS
    group = ny // width
    size = group // 2
    chunks = nz // size
    half = ny // 2
    row, col = lax.axis_index("row"), lax.axis_index("col")
    up, down = row > 0, row < n_row - 1
    left, right = col > 0, col < n_col - 1

    load_e = pltpu.make_async_copy(e_in, e_s.at[:, pl.ds(0, nz)], local_sem.at[0])
    load_h = pltpu.make_async_copy(h_in, h_s.at[:, pl.ds(1, nz)], local_sem.at[1])
    load_c = pltpu.make_async_copy(coef_in, coef_s, local_sem.at[2])
    load_e.start()
    load_h.start()
    load_c.start()
    n_modes = basis_in.shape[0]
    modes_3d = modes.reshape(n_modes * n_row, nx, ny)
    load_b = pltpu.make_async_copy(
        basis_in.at[:, pl.ds(pl.multiple_of(row * nx, nx), nx)],
        modes_3d.at[pl.ds(row * n_modes, n_modes)], local_sem.at[3])
    load_b.start()
    row_peers = [lax.rem(row + k, n_row) for k in range(1, n_row)]
    pair = lax.rem(col, 2)
    near = [
        {"row": lax.rem(row + k, n_row), "col": col - pair + lax.rem(pair + m, 2)}
        for k in range(n_row) for m in range(2) if k + m]
    far = [{"row": row, "col": lax.rem(col + 2 * k, n_col)} for k in range(1, n_col // 2)]
    other = col - 1 + 2 * pair
    beside = jnp.logical_and(other >= 0, other < n_col)
    part[...] = jnp.zeros_like(part)
    up_in[...] = jnp.zeros_like(up_in)
    down_in[...] = jnp.zeros_like(down_in)
    for side, there in enumerate((left, right)):
        @pl.when(jnp.logical_not(there))
        def _():
            y_in[side] = jnp.zeros(y_in.shape[1:], jnp.float32)

    barrier = pltpu.get_barrier_semaphore()
    for peer in near + far:
        pl.semaphore_signal(barrier, inc=1, device_id=peer, device_id_type=pl.DeviceIdType.MESH)

    @pl.when(beside)
    def _():
        pl.semaphore_signal(
            barrier, inc=1, device_id={"row": row, "col": other}, device_id_type=pl.DeviceIdType.MESH)

    zero = jnp.zeros((nx, ny), jnp.float32)
    for c in range(3):
        e_s[c, nz] = zero
        h_s[c, 0] = zero
        side_h[c, 0] = zero
        side_h[c, chunks + 1] = zero
        for k in range(2):
            side_e[c, chunks + k] = zero
            last_x[c, chunks + k] = zero
    for c in range(2):
        first_y[c, chunks] = zero
    down_out[chunks] = jnp.zeros(down_out.shape[1:], jnp.float32)

    def clear(z, carry):
        for k in range(8):
            psi[k, z] = zero
        return carry

    lax.fori_loop(0, nz, clear, 0)
    side_psi[...] = jnp.zeros_like(side_psi)
    row_psi[...] = jnp.zeros_like(row_psi)
    before[...] = jnp.zeros_like(before)
    before_psi[...] = jnp.zeros_like(before_psi)

    sub = lax.broadcasted_iota(jnp.int32, (nx, ny), 0)
    lane = lax.broadcasted_iota(jnp.int32, (nx, ny), 1)
    spot = lax.rem(lane, width)
    block = lax.div(lax.rem(lane, half), width)
    on_left = lane < half
    w = [jnp.full((nx, ny), width_ref[k], jnp.int32).astype(jnp.float32) for k in range(4)]
    x_pos = (sub + row * nx).astype(jnp.float32)
    y_pos = (lane + col * ny).astype(jnp.float32)
    x_before = (jnp.zeros_like(sub) + (row * nx - 1)).astype(jnp.float32)
    x_last = (jnp.zeros_like(sub) + (row * nx + nx - 1)).astype(jnp.float32)
    y_side = (spot + col * ny + jnp.where(on_left, -width, ny)).astype(jnp.float32)
    full_x, full_y = float(nx * n_row), float(ny * n_col)
    pairs = (
        absorber(x_pos + 0.5, full_x, w[0], w[1]), absorber(y_pos + 0.5, full_y, w[2], w[3]),
        absorber(x_pos, full_x, w[0], w[1]), absorber(y_pos, full_y, w[2], w[3]),
        absorber(x_before + 0.5, full_x, w[0], w[1]), absorber(x_last + 0.5, full_x, w[0], w[1]),
        absorber(y_side + 0.5, full_y, w[2], w[3]), absorber(y_side, full_y, w[2], w[3]),
    )
    for k, (damp, gain) in enumerate(pairs):
        prof[2 * k] = damp
        prof[2 * k + 1] = gain
    side_step = time_step * jnp.where(on_left, left.astype(jnp.float32), right.astype(jnp.float32))
    up_mask = up.astype(jnp.float32)

    routes = ((up, {"row": row - 1, "col": col}), (down, {"row": row + 1, "col": col}))
    arrives = (down, up)
    rows = 2 * size + 2

    def copy_of(m, slot, k):
        src, dst = ((up_out, up_in), (down_out, down_in))[m]
        return pltpu.make_async_remote_copy(
            src_ref=src.at[k, pl.ds(0, rows)], dst_ref=dst.at[slot, k, pl.ds(0, rows)],
            send_sem=x_send.at[m, slot, k], recv_sem=x_recv.at[m, slot, k],
            device_id=routes[m][1], device_id_type=pl.DeviceIdType.MESH)

    def start(m, slot, k):
        @pl.when(routes[m][0])
        def _():
            copy_of(m, slot, k).start()

    def wait_recv(m, slot, k):
        @pl.when(arrives[m])
        def _():
            copy_of(m, slot, k).wait_recv()

    def wait_send(m, slot, k):
        @pl.when(routes[m][0])
        def _():
            copy_of(m, slot, k).wait_send()

    sides = ((left, {"row": row, "col": col - 1}), (right, {"row": row, "col": col + 1}))

    def y_copy(side, arriving, part):
        parts = (pl.ds(0, 6), pl.ds(6, 1))[part]
        a = 1 - side if arriving else side
        return pltpu.make_async_remote_copy(
            src_ref=y_out.at[a, parts], dst_ref=y_in.at[1 - a, parts], send_sem=y_send.at[a, part],
            recv_sem=y_recv.at[1 - a, part], device_id=sides[side][1], device_id_type=pl.DeviceIdType.MESH)

    def y_wait(part):
        for side in range(2):
            @pl.when(sides[side][0])
            def _():
                y_copy(side, True, part).wait_recv()

    load_e.wait()
    load_h.wait()
    load_c.wait()

    def plane(c, z):
        return e_s[c, z] if c < 3 else h_s[c - 3, z + 1] if c < 6 else coef_s[z]

    def pack_sides(q, carry):
        for c in range(7):
            first, last = zero, zero
            for i in range(group):
                value = plane(c, q * group + i)
                here = lax.div(lane, width) == i
                first = jnp.where(here, pltpu.roll(value, i * width, 1) if i else value, first)
                last = jnp.where(here, pltpu.roll(value, (i * width + width) % ny, 1) if (i + 1) % group else value, last)
            y_out[0, c, q] = first
            y_out[1, c, q] = last
        return carry

    lax.fori_loop(0, nz // group, pack_sides, 0)
    pl.semaphore_wait(barrier, len(near) + len(far) + beside.astype(jnp.int32))
    for side in range(2):
        @pl.when(sides[side][0])
        def _():
            for part_no in range(2):
                y_copy(side, False, part_no).start()

    def first_pack(k, carry):
        fx, fz = zero, zero
        for j in range(size):
            z = k * size + j
            ex, ey, ez = e_s[0, z], e_s[1, z], e_s[2, z]
            hy, hz = h_s[1, z + 1], h_s[2, z + 1]
            up_out[k, j:j + 1, :] = ey[0:1]
            up_out[k, size + j:size + j + 1, :] = ez[0:1]
            down_out[k, j:j + 1, :] = hy[nx - 1:nx]
            down_out[k, size + j:size + j + 1, :] = hz[nx - 1:nx]
            for c, value in enumerate((ex, ey, ez)):
                last_x[c, k, j:j + 1, :] = value[nx - 1:nx]
            at = lane == j * width + width - 1
            fx = jnp.where(at, pltpu.roll(ex, j * width + width - 1, 1), fx)
            fz = jnp.where(at, pltpu.roll(ez, j * width + width - 1, 1), fz)
        first_y[0, k] = fx
        first_y[1, k] = fz
        return carry

    lax.fori_loop(0, chunks, first_pack, 0)

    y_wait(0)

    def unpack(comps, q, carry):
        for c in comps:
            a, b = y_in[0, c, q], y_in[1, c, q]
            values = jnp.where(on_left, a, pltpu.roll(b, half, 1)), jnp.where(on_left, pltpu.roll(a, half, 1), b)
            for i in range(2):
                if c < 3:
                    side_e[c, 2 * q + i] = values[i]
                elif c < 6:
                    side_h[c - 3, 2 * q + i + 1] = values[i]
                else:
                    side_coef[2 * q + i] = values[i]
        return carry

    lax.fori_loop(0, nz // group, functools.partial(unpack, range(6)), 0)

    def z_after(here, after):
        return jnp.where(block == size - 1, pltpu.roll(after, half - width, 1), pltpu.roll(here, ny - width, 1))

    def z_before(here, prior):
        return jnp.where(block == 0, pltpu.roll(prior, half + width, 1), pltpu.roll(here, width, 1))

    def y_after(here, edge):
        return jnp.where(spot == width - 1, edge, pltpu.roll(here, ny - 1, 1))

    def y_before(here, edge):
        return jnp.where(spot == 0, edge, pltpu.roll(here, 1, 1))

    def spread(value):
        return jnp.broadcast_to(value, (nx, ny))

    def below_main(k):
        ex, ey, ez = last_x[0, k], last_x[1, k], last_x[2, k]
        hdy, hgy, ldx, lgx = prof[2], prof[3], prof[10], prof[11]
        ex_dz = jnp.where(sub == nx - 1, spread(last_x[0, k + 1, 0:1, :]), pltpu.roll(ex, nx - 1, 0)) - ex
        corner = jnp.where(lane == half + width * sub, spread(side_e[0, k, nx - 1:nx, :]), 0.0)
        corner = jnp.sum(corner, axis=1, keepdims=True)
        ex_dy = jnp.where(lane == ny - 1, corner, pltpu.roll(ex, ny - 1, 1)) - ex
        p1 = ldx * row_psi[0, k] - lgx * ez
        p2 = ldx * row_psi[1, k] - lgx * ey
        p3 = hdy * row_psi[2, k] + hgy * ex_dy
        row_psi[0, k], row_psi[1, k], row_psi[2, k] = p1, p2, p3
        down_out[k, 0:size, :] = down_out[k, 0:size, :] - time_step * (ex_dz + ez - p1)
        down_out[k, size:2 * size, :] = down_out[k, size:2 * size, :] - time_step * (p2 - ey - ex_dy - p3)
    def below_side(k):
        ex, ey, ez = side_e[0, k], side_e[1, k], side_e[2, k]
        hdx, hgx, hdy, hgy = prof[0], prof[1], prof[12], prof[13]
        ex_dz = z_after(ex, side_e[0, k + 1]) - ex
        ex_dy = y_after(ex, first_y[0, k]) - ex
        p1 = hdx * side_psi[1, k] - hgx * ez
        p2 = hdx * side_psi[2, k] - hgx * ey
        p3 = hdy * side_psi[3, k] + hgy * ex_dy
        hy = side_h[1, k + 1] - side_step * (ex_dz + ez - p1)
        hz = side_h[2, k + 1] - side_step * (p2 - ey - ex_dy - p3)
        down_out[k, 2 * size:2 * size + 1, :] = hy[nx - 1:nx]
        down_out[k, 2 * size + 1:2 * size + 2, :] = hz[nx - 1:nx]

    def first_send(k, carry):
        up_out[k, 2 * size:2 * size + 1, :] = side_e[1, k, 0:1, :]
        up_out[k, 2 * size + 1:2 * size + 2, :] = side_e[2, k, 0:1, :]
        start(0, 0, k)
        below_main(k)
        below_side(k)
        start(1, 0, k)
        return carry

    lax.fori_loop(0, chunks, first_send, 0)
    y_wait(1)
    lax.fori_loop(0, nz // group, functools.partial(unpack, range(6, 7)), 0)
    piece = n_modes // STEPS

    def mode_copies(s):
        return [
            pltpu.make_async_remote_copy(
                src_ref=basis_in.at[pl.ds(s * piece, piece), pl.ds(pl.multiple_of(peer * nx, nx), nx)],
                dst_ref=modes_3d.at[pl.ds(row * n_modes + s * piece, piece)],
                send_sem=mode_send.at[k, s], recv_sem=mode_recv.at[k, s],
                device_id={"row": peer, "col": col}, device_id_type=pl.DeviceIdType.MESH)
            for k, peer in enumerate(row_peers)
        ]

    def side_magnetic(slot, k):
        hdx, hgx = prof[0], prof[1]
        sdy, sgy = prof[12], prof[13]
        ex, ey, ez = side_e[0, k], side_e[1, k], side_e[2, k]
        row_y = spread(up_in[slot, k, 2 * size:2 * size + 1, :])
        row_z = spread(up_in[slot, k, 2 * size + 1:2 * size + 2, :])
        ey_dz = z_after(ey, side_e[1, k + 1]) - ey
        ex_dz = z_after(ex, side_e[0, k + 1]) - ex
        ez_dy = y_after(ez, first_y[1, k]) - ez
        ex_dy = y_after(ex, first_y[0, k]) - ex
        ez_dx = jnp.where(sub == nx - 1, row_z, pltpu.roll(ez, nx - 1, 0)) - ez
        ey_dx = jnp.where(sub == nx - 1, row_y, pltpu.roll(ey, nx - 1, 0)) - ey
        p0 = sdy * side_psi[0, k] + sgy * ez_dy
        p1 = hdx * side_psi[1, k] + hgx * ez_dx
        p2 = hdx * side_psi[2, k] + hgx * ey_dx
        p3 = sdy * side_psi[3, k] + sgy * ex_dy
        side_psi[0, k], side_psi[1, k], side_psi[2, k], side_psi[3, k] = p0, p1, p2, p3
        side_hx = side_h[0, k + 1] - side_step * (ez_dy + p0 - ey_dz)
        side_hy = side_h[1, k + 1] - side_step * (ex_dz - ez_dx - p1)
        side_hz = side_h[2, k + 1] - side_step * (ey_dx + p2 - ex_dy - p3)
        side_h[0, k + 1], side_h[1, k + 1], side_h[2, k + 1] = side_hx, side_hy, side_hz

    def tick(s, slot, k):
        more = s < STEPS - 1
        hdx, hgx, hdy, hgy = prof[0], prof[1], prof[2], prof[3]
        edx, egx, edy, egy = prof[4], prof[5], prof[6], prof[7]
        bdx, bgx = prof[8], prof[9]
        prior = jnp.where(k > 0, k - 1, chunks)
        wait_recv(0, slot, k)
        wait_recv(1, slot, k)
        wait_send(0, slot, k)

        @pl.when(k > 0)
        def _():
            wait_send(1, slot, k - 1)

        side_magnetic(slot, k)
        edge_ex, edge_ez = side_e[0, k], side_e[2, k]
        side_hx, side_hy, side_hz = side_h[0, k + 1], side_h[1, k + 1], side_h[2, k + 1]
        ey, ez = up_out[k, 0:size, :], up_out[k, size:2 * size, :]
        p1 = bdx * before_psi[0, k] + bgx * ez
        p2 = bdx * before_psi[1, k] + bgx * ey
        before_psi[0, k], before_psi[1, k] = p1, p2
        hy = before[0, k] + time_step * (ez + p1)
        hz = before[1, k] - time_step * (ey + p2)
        before[0, k], before[1, k] = hy, hz
        ey, ez = up_out[k, 2 * size:2 * size + 1, :], up_out[k, 2 * size + 1:2 * size + 2, :]
        factor = side_step[0:1] * (1.0 + bgx[0:1])
        before_h[0:size, :] = up_mask * (hy + down_in[slot, k, 0:size, :])
        before_h[size:2 * size, :] = up_mask * (hz + down_in[slot, k, size:2 * size, :])
        back_y = up_mask * (down_in[slot, k, 2 * size:2 * size + 1, :] + factor * ez)
        back_z = up_mask * (down_in[slot, k, 2 * size + 1:2 * size + 2, :] - factor * ey)

        last_hx, last_hz, first_ex, first_ez = zero, zero, zero, zero
        below_hx, below_hy = h_s[0, k * size], h_s[1, k * size]
        ex, ey, ez = e_s[0, k * size], e_s[1, k * size], e_s[2, k * size]
        for j in range(size):
            z = k * size + j
            next_ex, next_ey, next_ez = e_s[0, z + 1], e_s[1, z + 1], e_s[2, z + 1]
            row_y = spread(up_in[slot, k, j:j + 1, :])
            row_z = spread(up_in[slot, k, size + j:size + j + 1, :])
            to_end = (ny - 1 - half - width * j) % ny
            col_x = pltpu.roll(edge_ex, to_end, 1)
            col_z = pltpu.roll(edge_ez, to_end, 1)
            ey_dz = next_ey - ey
            ex_dz = next_ex - ex
            ez_dy = jnp.where(lane == ny - 1, col_z, pltpu.roll(ez, ny - 1, 1)) - ez
            ex_dy = jnp.where(lane == ny - 1, col_x, pltpu.roll(ex, ny - 1, 1)) - ex
            ez_dx = jnp.where(sub == nx - 1, row_z, pltpu.roll(ez, nx - 1, 0)) - ez
            ey_dx = jnp.where(sub == nx - 1, row_y, pltpu.roll(ey, nx - 1, 0)) - ey
            p0 = hdy * psi[0, z] + hgy * ez_dy
            p1 = hdx * psi[1, z] + hgx * ez_dx
            p2 = hdx * psi[2, z] + hgx * ey_dx
            p3 = hdy * psi[3, z] + hgy * ex_dy
            psi[0, z], psi[1, z], psi[2, z], psi[3, z] = p0, p1, p2, p3
            hx = h_s[0, z + 1] - time_step * (ez_dy + p0 - ey_dz)
            hy = h_s[1, z + 1] - time_step * (ex_dz - ez_dx - p1)
            hz = h_s[2, z + 1] - time_step * (ey_dx + p2 - ex_dy - p3)
            h_s[0, z + 1], h_s[1, z + 1], h_s[2, z + 1] = hx, hy, hz
            at = lane == half + width * j
            last_hx = jnp.where(at, pltpu.roll(hx, (half + width * j + 1) % ny, 1), last_hx)
            last_hz = jnp.where(at, pltpu.roll(hz, (half + width * j + 1) % ny, 1), last_hz)

            row_y = spread(before_h[j:j + 1, :])
            row_z = spread(before_h[size + j:size + j + 1, :])
            to_start = ny - (width * j + width - 1)
            col_x = pltpu.roll(side_hx, to_start, 1)
            col_z = pltpu.roll(side_hz, to_start, 1)
            hy_dz = hy - below_hy
            hx_dz = hx - below_hx
            hz_dy = hz - jnp.where(lane == 0, col_z, pltpu.roll(hz, 1, 1))
            hx_dy = hx - jnp.where(lane == 0, col_x, pltpu.roll(hx, 1, 1))
            hz_dx = hz - jnp.where(sub == 0, row_z, pltpu.roll(hz, 1, 0))
            hy_dx = hy - jnp.where(sub == 0, row_y, pltpu.roll(hy, 1, 0))
            p0 = edy * psi[4, z] + egy * hz_dy
            p1 = edx * psi[5, z] + egx * hz_dx
            p2 = edx * psi[6, z] + egx * hy_dx
            p3 = edy * psi[7, z] + egy * hx_dy
            psi[4, z], psi[5, z], psi[6, z], psi[7, z] = p0, p1, p2, p3
            amount = coef_s[z]
            ex = ex + amount * (hz_dy + p0 - hy_dz)
            ey = ey + amount * (hx_dz - hz_dx - p1)
            ez = ez + amount * (hy_dx + p2 - hx_dy - p3)
            e_s[0, z], e_s[1, z], e_s[2, z] = ex, ey, ez
            at = lane == width * j + width - 1
            first_ex = jnp.where(at, pltpu.roll(ex, width * j + width - 1, 1), first_ex)
            first_ez = jnp.where(at, pltpu.roll(ez, width * j + width - 1, 1), first_ez)
            up_out[k, j:j + 1, :] = ey[0:1]
            up_out[k, size + j:size + j + 1, :] = ez[0:1]
            for c, value in enumerate((ex, ey, ez)):
                last_x[c, k, j:j + 1, :] = value[nx - 1:nx]
            below_hx, below_hy = hx, hy
            ex, ey, ez = next_ex, next_ey, next_ez
        first_y[0, k] = first_ex
        first_y[1, k] = first_ez
        below_main(prior)

        sdy, sgy = prof[14], prof[15]
        hx, hy, hz = side_hx, side_hy, side_hz
        hy_dz = hy - z_before(hy, side_h[1, k])
        hx_dz = hx - z_before(hx, side_h[0, k])
        hz_dy = hz - y_before(hz, last_hz)
        hx_dy = hx - y_before(hx, last_hx)
        hz_dx = hz - jnp.where(sub == 0, spread(back_z), pltpu.roll(hz, 1, 0))
        hy_dx = hy - jnp.where(sub == 0, spread(back_y), pltpu.roll(hy, 1, 0))
        p0 = sdy * side_psi[4, k] + sgy * hz_dy
        p1 = edx * side_psi[5, k] + egx * hz_dx
        p2 = edx * side_psi[6, k] + egx * hy_dx
        p3 = sdy * side_psi[7, k] + sgy * hx_dy
        side_psi[4, k], side_psi[5, k], side_psi[6, k], side_psi[7, k] = p0, p1, p2, p3
        amount = side_coef[k]
        ex = side_e[0, k] + amount * (hz_dy + p0 - hy_dz)
        ey = side_e[1, k] + amount * (hx_dz - hz_dx - p1)
        ez = side_e[2, k] + amount * (hy_dx + p2 - hx_dy - p3)
        side_e[0, k], side_e[1, k], side_e[2, k] = ex, ey, ez
        up_out[k, 2 * size:2 * size + 1, :] = ey[0:1]
        up_out[k, 2 * size + 1:2 * size + 2, :] = ez[0:1]

        below_side(prior)

        @pl.when(more)
        def _():
            start(0, 1 - slot, k)

        @pl.when(jnp.logical_and(more, k > 0))
        def _():
            start(1, 1 - slot, k - 1)

    def step(s, carry):
        slot = lax.rem(s, 2)
        def body(k, carry):
            tick(s, slot, k)
            return carry

        lax.fori_loop(0, chunks, body, 0)
        wait_send(1, slot, chunks - 1)

        @pl.when(s < STEPS - 1)
        def _():
            below_main(chunks - 1)
            below_side(chunks - 1)
            start(1, 1 - slot, chunks - 1)

        @pl.when(s < STEPS - 1)
        def _():
            for copy in mode_copies(s):
                copy.start()

        @pl.when(s == STEPS - 2)
        def _():
            for copy in mode_copies(STEPS - 1):
                copy.start()

        return carry

    lax.fori_loop(0, STEPS, step, 0)
    for side in range(2):
        @pl.when(sides[side][0])
        def _():
            for part_no in range(2):
                y_copy(side, False, part_no).wait_send()

    count = snaps.shape[0] // nx

    def pick(s, carry):
        planes = []
        for j in range(8):
            index = index_ref[s * 8 + j]
            c = index // nz
            z = index - c * nz
            e_plane = e_s[jnp.minimum(c, 2), z]
            h_plane = h_s[jnp.maximum(c - 3, 0), z + 1]
            planes.append(jnp.where(c < 3, e_plane, h_plane))
        for j in range(8):
            snaps[pl.ds(pl.multiple_of((s * 8 + j) * nx, nx), nx), :] = planes[j]
        return carry

    lax.fori_loop(0, count // 8, pick, 0)
    load_b.wait()

    def wait_modes(s, carry):
        for copy in mode_copies(s):
            copy.wait()
        return carry

    lax.fori_loop(0, STEPS, wait_modes, 0)
    n_all = modes.shape[0] // nx
    dims = (((1,), (1,)), ((), ()))
    proj, gram = None, None
    for x in range(nx):
        a = snaps[pl.ds(x, count, stride=nx), :]
        b = modes[pl.ds(x, n_all, stride=nx), :]
        p = lax.dot_general(a, b, dims, precision=lax.Precision.HIGHEST, preferred_element_type=jnp.float32)
        g = lax.dot_general(a, a, dims, precision=lax.Precision.HIGHEST, preferred_element_type=jnp.float32)
        proj, gram = (p, g) if x == 0 else (proj + p, gram + g)
    gram = gram / float(nx * n_row * ny * n_col)
    share = part.shape[1]
    for k in range(part.shape[0]):
        part[k, :, 0:n_all] = proj[k * share:(k + 1) * share]
        part[k, :, n_all:n_all + count] = gram[k * share:(k + 1) * share]
    own = 2 * row + pair

    def exchange(peers, src_of, dst, sends, recvs):
        result = []
        for k, peer in enumerate(peers):
            result.append(pltpu.make_async_remote_copy(
                src_ref=src_of(peer), dst_ref=dst, send_sem=sends.at[k], recv_sem=recvs.at[k],
                device_id=peer, device_id_type=pl.DeviceIdType.MESH))
        for copy in result:
            copy.start()
        for copy in result:
            copy.wait()

    row_sums[own] = part[own]
    exchange(
        near, lambda peer: part.at[2 * peer["row"] + lax.rem(peer["col"], 2)],
        row_sums.at[own], sum_send, sum_recv)
    value = row_sums[0]
    for k in range(1, 2 * n_row):
        value = value + row_sums[k]
    level = lax.div(col, 2)
    col_sums[level] = value
    exchange(far, lambda peer: col_sums.at[level], col_sums.at[level], col_send, col_recv)
    value = col_sums[0]
    for k in range(1, n_col // 2):
        value = value + col_sums[k]
    total[own] = value
    exchange(near, lambda peer: total.at[own], total.at[own], back_send, back_recv)


def write_kernel(e_s, h_s, total, e_out, h_out, proj_out, gram_out, proj, gram, sems):
    nz = e_out.shape[1]
    copies = [
        pltpu.make_async_copy(e_s.at[:, pl.ds(0, nz)], e_out, sems.at[0]),
        pltpu.make_async_copy(h_s.at[:, pl.ds(1, nz)], h_out, sems.at[1]),
        pltpu.make_async_copy(proj, proj_out, sems.at[2]), pltpu.make_async_copy(gram, gram_out, sems.at[3]),
    ]
    copies[0].start()
    copies[1].start()
    n_all, count = proj.shape[1], gram.shape[1]
    share = total.shape[1]
    for k in range(total.shape[0]):
        proj[k * share:(k + 1) * share, :] = total[k, :, 0:n_all]
        gram[k * share:(k + 1) * share, :] = total[k, :, n_all:n_all + count]
    copies[2].start()
    copies[3].start()
    for copy in copies:
        copy.wait()


def shards(e_field, h_field, e_coef, basis, pml_width, snap_index):
    nz, nx, ny = e_coef.shape
    n_row, n_col = lax.axis_size("row"), lax.axis_size("col")
    modes, count = basis.shape[0] * n_row, snap_index.shape[0]
    f32 = jnp.float32
    size = ny // STEPS // 2
    chunks = nz // size
    wide = modes + (count + 127) // 128 * 128
    any_space = pl.BlockSpec(memory_space=pltpu.HBM)
    smem, vmem = pl.BlockSpec(memory_space=pltpu.SMEM), pl.BlockSpec(memory_space=pltpu.VMEM)
    held = pltpu.VMEM((3, nz + 1, nx, ny), f32)
    share = count // (2 * n_row)
    e_s, h_s, total = pl.pallas_call(
        functools.partial(step_kernel, n_row, n_col),
        out_shape=[held, held, pltpu.VMEM((2 * n_row, share, wide), f32)],
        in_specs=[smem, smem, any_space, any_space, any_space, any_space],
        out_specs=[vmem, vmem, vmem],
        scratch_shapes=[
            pltpu.VMEM((nz, nx, ny), f32), pltpu.VMEM((8, nz, nx, ny), f32),
            pltpu.VMEM((3, chunks + 2, nx, ny), f32), pltpu.VMEM((3, chunks + 2, nx, ny), f32),
            pltpu.VMEM((chunks, nx, ny), f32), pltpu.VMEM((8, chunks + 1, nx, ny), f32),
            pltpu.VMEM((2, chunks + 1, nx, ny), f32),
            pltpu.VMEM((2, 7, chunks // 2, nx, ny), f32), pltpu.VMEM((2, 7, chunks // 2, nx, ny), f32),
            pltpu.VMEM((chunks, 3 * size, ny), f32), pltpu.VMEM((2, chunks, 3 * size, ny), f32),
            pltpu.VMEM((chunks + 1, 3 * size, ny), f32), pltpu.VMEM((2, chunks, 3 * size, ny), f32),
            pltpu.VMEM((3, chunks + 2, size, ny), f32), pltpu.VMEM((3, chunks + 1, size, ny), f32),
            pltpu.VMEM((2, chunks, size, ny), f32), pltpu.VMEM((2, chunks, size, ny), f32),
            pltpu.VMEM((2 * size, ny), f32),
            pltpu.VMEM((16, nx, ny), f32),
            pltpu.VMEM((modes * nx, ny), f32), pltpu.VMEM((count * nx, ny), f32),
            pltpu.VMEM((2 * n_row, share, wide), f32), pltpu.VMEM((2 * n_row, share, wide), f32),
            pltpu.VMEM((n_col // 2, share, wide), f32),
            pltpu.SemaphoreType.DMA((4,)),
            pltpu.SemaphoreType.DMA((2, 2)), pltpu.SemaphoreType.DMA((2, 2)),
            pltpu.SemaphoreType.DMA((2, 2, chunks)), pltpu.SemaphoreType.DMA((2, 2, chunks)),
            pltpu.SemaphoreType.DMA((n_row - 1, STEPS)), pltpu.SemaphoreType.DMA((n_row - 1, STEPS)),
            pltpu.SemaphoreType.DMA((2 * n_row - 1,)), pltpu.SemaphoreType.DMA((2 * n_row - 1,)),
            pltpu.SemaphoreType.DMA((n_col // 2 - 1,)), pltpu.SemaphoreType.DMA((n_col // 2 - 1,)),
            pltpu.SemaphoreType.DMA((2 * n_row - 1,)), pltpu.SemaphoreType.DMA((2 * n_row - 1,)),
        ],
        compiler_params=pltpu.CompilerParams(
            collective_id=0, has_side_effects=True, vmem_limit_bytes=65_280_000
        ),
    )(pml_width, snap_index, e_field, h_field, e_coef, basis)
    return pl.pallas_call(
        write_kernel,
        out_shape=[
            jax.ShapeDtypeStruct(e_field.shape, f32), jax.ShapeDtypeStruct(h_field.shape, f32),
            jax.ShapeDtypeStruct((count, modes), f32), jax.ShapeDtypeStruct((count, count), f32),
        ],
        in_specs=[vmem, vmem, vmem],
        out_specs=[any_space, any_space, any_space, any_space],
        scratch_shapes=[
            pltpu.VMEM((count, modes), f32), pltpu.VMEM((count, count), f32), pltpu.SemaphoreType.DMA((4,)),
        ],
        compiler_params=pltpu.CompilerParams(vmem_limit_bytes=16_777_216),
    )(e_s, h_s, total)


def solution(mesh):
    in_specs = (
        P(None, None, "row", "col"),
        P(None, None, "row", "col"),
        P(None, "row", "col"),
        P("row", None, "col"),
        P(),
        P(),
    )
    out_specs = (P(None, None, "row", "col"), P(None, None, "row", "col"), P(), P())
    return jax.shard_map(shards, mesh=mesh, in_specs=in_specs, out_specs=out_specs, check_vma=False)
```

```python
import functools
import jax
import jax.numpy as jnp
from jax import lax
from jax.experimental import pallas as pl
from jax.experimental.pallas import tpu as pltpu
from jax.sharding import PartitionSpec as P

STEPS = 8


time_step = 0.5
sigma_top = 4.0
alpha_shift = 0.05


def absorber(positions, total, low, high):
    depth = jnp.maximum(
        jnp.maximum((low - positions) / low, (positions - (total - 1.0 - high)) / high), 0.0
    )
    sigma = sigma_top * (depth * depth * depth)
    damp = jnp.exp(-(sigma + alpha_shift) * time_step)
    gain = sigma / (sigma + alpha_shift) * (damp - 1.0)
    return damp, gain


def step_kernel(
    n_row, n_col, width_ref, index_ref, e_in, h_in, coef_in, basis_in, e_s, h_s, total,
    coef_s, psi, side_e, side_h, side_coef, side_psi, first_y, y_out, y_in,
    up_out, up_in, down_out, down_in, last_x, row_psi, before, before_psi, before_h,
    prof, modes, snaps, part, row_sums, col_sums,
    local_sem, y_send, y_recv, x_send, x_recv, mode_send, mode_recv,
    sum_send, sum_recv, col_send, col_recv, back_send, back_recv,
):
    nz, nx, ny = coef_s.shape
    width = STEPS
    group = ny // width
    size = group // 2
    chunks = nz // size
    half = ny // 2
    row, col = lax.axis_index("row"), lax.axis_index("col")
    up, down = row > 0, row < n_row - 1
    left, right = col > 0, col < n_col - 1

    load_e = pltpu.make_async_copy(e_in, e_s.at[:, pl.ds(0, nz)], local_sem.at[0])
    load_h = pltpu.make_async_copy(h_in, h_s.at[:, pl.ds(1, nz)], local_sem.at[1])
    load_c = pltpu.make_async_copy(coef_in, coef_s, local_sem.at[2])
    load_e.start()
    load_h.start()
    load_c.start()
    n_modes = basis_in.shape[0]
    modes_3d = modes.reshape(n_modes * n_row, nx, ny)
    load_b = pltpu.make_async_copy(
        basis_in.at[:, pl.ds(pl.multiple_of(row * nx, nx), nx)],
        modes_3d.at[pl.ds(row * n_modes, n_modes)], local_sem.at[3])
    load_b.start()
    row_peers = [lax.rem(row + k, n_row) for k in range(1, n_row)]
    pair = lax.rem(col, 2)
    near = [
        {"row": lax.rem(row + k, n_row), "col": col - pair + lax.rem(pair + m, 2)}
        for k in range(n_row) for m in range(2) if k + m]
    far = [{"row": row, "col": lax.rem(col + 2 * k, n_col)} for k in range(1, n_col // 2)]
    other = col - 1 + 2 * pair
    beside = jnp.logical_and(other >= 0, other < n_col)
    up_in[...] = jnp.zeros_like(up_in)
    down_in[...] = jnp.zeros_like(down_in)
    for side, there in enumerate((left, right)):
        @pl.when(jnp.logical_not(there))
        def _():
            y_in[side] = jnp.zeros(y_in.shape[1:], jnp.float32)

    barrier = pltpu.get_barrier_semaphore()
    for peer in near + far:
        pl.semaphore_signal(barrier, inc=1, device_id=peer, device_id_type=pl.DeviceIdType.MESH)

    @pl.when(beside)
    def _():
        pl.semaphore_signal(
            barrier, inc=1, device_id={"row": row, "col": other}, device_id_type=pl.DeviceIdType.MESH)

    zero = jnp.zeros((nx, ny), jnp.float32)
    for c in range(3):
        e_s[c, nz] = zero
        h_s[c, 0] = zero
        side_h[c, 0] = zero
        side_h[c, chunks + 1] = zero
        for k in range(2):
            side_e[c, chunks + k] = zero
            last_x[c, chunks + k] = zero
    for c in range(2):
        first_y[c, chunks] = zero
    down_out[chunks] = jnp.zeros(down_out.shape[1:], jnp.float32)

    def clear(z, carry):
        for k in range(8):
            psi[k, z] = zero
        return carry

    lax.fori_loop(0, nz, clear, 0)
    side_psi[...] = jnp.zeros_like(side_psi)
    row_psi[...] = jnp.zeros_like(row_psi)
    before[...] = jnp.zeros_like(before)
    before_psi[...] = jnp.zeros_like(before_psi)

    sub = lax.broadcasted_iota(jnp.int32, (nx, ny), 0)
    lane = lax.broadcasted_iota(jnp.int32, (nx, ny), 1)
    spot = lax.rem(lane, width)
    block = lax.div(lax.rem(lane, half), width)
    on_left = lane < half
    w = [jnp.full((nx, ny), width_ref[k], jnp.int32).astype(jnp.float32) for k in range(4)]
    x_pos = (sub + row * nx).astype(jnp.float32)
    y_pos = (lane + col * ny).astype(jnp.float32)
    x_before = (jnp.zeros_like(sub) + (row * nx - 1)).astype(jnp.float32)
    x_last = (jnp.zeros_like(sub) + (row * nx + nx - 1)).astype(jnp.float32)
    y_side = (spot + col * ny + jnp.where(on_left, -width, ny)).astype(jnp.float32)
    full_x, full_y = float(nx * n_row), float(ny * n_col)
    pairs = (
        absorber(x_pos + 0.5, full_x, w[0], w[1]), absorber(y_pos + 0.5, full_y, w[2], w[3]),
        absorber(x_pos, full_x, w[0], w[1]), absorber(y_pos, full_y, w[2], w[3]),
        absorber(x_before + 0.5, full_x, w[0], w[1]), absorber(x_last + 0.5, full_x, w[0], w[1]),
        absorber(y_side + 0.5, full_y, w[2], w[3]), absorber(y_side, full_y, w[2], w[3]),
    )
    for k, (damp, gain) in enumerate(pairs):
        prof[2 * k] = damp
        prof[2 * k + 1] = gain
    side_step = time_step * jnp.where(on_left, left.astype(jnp.float32), right.astype(jnp.float32))
    up_mask = up.astype(jnp.float32)

    routes = ((up, {"row": row - 1, "col": col}), (down, {"row": row + 1, "col": col}))
    arrives = (down, up)
    rows = 2 * size + 2

    def copy_of(m, slot, k):
        src, dst = ((up_out, up_in), (down_out, down_in))[m]
        return pltpu.make_async_remote_copy(
            src_ref=src.at[k, pl.ds(0, rows)], dst_ref=dst.at[slot, k, pl.ds(0, rows)],
            send_sem=x_send.at[m, slot, k], recv_sem=x_recv.at[m, slot, k],
            device_id=routes[m][1], device_id_type=pl.DeviceIdType.MESH)

    def start(m, slot, k):
        @pl.when(routes[m][0])
        def _():
            copy_of(m, slot, k).start()

    def wait_recv(m, slot, k):
        @pl.when(arrives[m])
        def _():
            copy_of(m, slot, k).wait_recv()

    def wait_send(m, slot, k):
        @pl.when(routes[m][0])
        def _():
            copy_of(m, slot, k).wait_send()

    sides = ((left, {"row": row, "col": col - 1}), (right, {"row": row, "col": col + 1}))

    def y_copy(side, arriving, q):
        a = 1 - side if arriving else side
        return pltpu.make_async_remote_copy(
            src_ref=y_out.at[a, q], dst_ref=y_in.at[1 - a, q], send_sem=y_send.at[a, q],
            recv_sem=y_recv.at[1 - a, q], device_id=sides[side][1], device_id_type=pl.DeviceIdType.MESH)

    def y_each(act, q):
        for side in range(2):
            @pl.when(sides[side][0])
            def _():
                act(side, q)

    load_e.wait()
    load_h.wait()
    load_c.wait()

    def plane(c, z):
        return e_s[c, z] if c < 3 else h_s[c - 3, z + 1] if c < 6 else coef_s[z]

    def pack_sides(q, carry):
        for c in range(7):
            first, last = zero, zero
            for i in range(group):
                value = plane(c, q * group + i)
                here = lax.div(lane, width) == i
                first = jnp.where(here, pltpu.roll(value, i * width, 1) if i else value, first)
                last = jnp.where(here, pltpu.roll(value, (i * width + width) % ny, 1) if (i + 1) % group else value, last)
            y_out[0, q, c] = first
            y_out[1, q, c] = last
        return carry

    lax.fori_loop(0, nz // group, pack_sides, 0)
    pl.semaphore_wait(barrier, len(near) + len(far) + beside.astype(jnp.int32))
    def y_start(q, carry):
        y_each(lambda side, q: y_copy(side, False, q).start(), q)
        return carry

    lax.fori_loop(0, nz // group, y_start, 0)

    def first_pack(k, carry):
        fx, fz = zero, zero
        for j in range(size):
            z = k * size + j
            ex, ey, ez = e_s[0, z], e_s[1, z], e_s[2, z]
            hy, hz = h_s[1, z + 1], h_s[2, z + 1]
            up_out[k, j:j + 1, :] = ey[0:1]
            up_out[k, size + j:size + j + 1, :] = ez[0:1]
            down_out[k, j:j + 1, :] = hy[nx - 1:nx]
            down_out[k, size + j:size + j + 1, :] = hz[nx - 1:nx]
            for c, value in enumerate((ex, ey, ez)):
                last_x[c, k, j:j + 1, :] = value[nx - 1:nx]
            at = lane == j * width + width - 1
            fx = jnp.where(at, pltpu.roll(ex, j * width + width - 1, 1), fx)
            fz = jnp.where(at, pltpu.roll(ez, j * width + width - 1, 1), fz)
        first_y[0, k] = fx
        first_y[1, k] = fz
        return carry

    lax.fori_loop(0, chunks, first_pack, 0)

    def unpack(q):
        for c in range(7):
            a, b = y_in[0, q, c], y_in[1, q, c]
            values = jnp.where(on_left, a, pltpu.roll(b, half, 1)), jnp.where(on_left, pltpu.roll(a, half, 1), b)
            for i in range(2):
                if c < 3:
                    side_e[c, 2 * q + i] = values[i]
                elif c < 6:
                    side_h[c - 3, 2 * q + i + 1] = values[i]
                else:
                    side_coef[2 * q + i] = values[i]

    def z_after(here, after):
        return jnp.where(block == size - 1, pltpu.roll(after, half - width, 1), pltpu.roll(here, ny - width, 1))

    def z_before(here, prior):
        return jnp.where(block == 0, pltpu.roll(prior, half + width, 1), pltpu.roll(here, width, 1))

    def y_after(here, edge):
        return jnp.where(spot == width - 1, edge, pltpu.roll(here, ny - 1, 1))

    def y_before(here, edge):
        return jnp.where(spot == 0, edge, pltpu.roll(here, 1, 1))

    def spread(value):
        return jnp.broadcast_to(value, (nx, ny))

    def below_main(k):
        ex, ey, ez = last_x[0, k], last_x[1, k], last_x[2, k]
        hdy, hgy, ldx, lgx = prof[2], prof[3], prof[10], prof[11]
        ex_dz = jnp.where(sub == nx - 1, spread(last_x[0, k + 1, 0:1, :]), pltpu.roll(ex, nx - 1, 0)) - ex
        corner = jnp.where(lane == half + width * sub, spread(side_e[0, k, nx - 1:nx, :]), 0.0)
        corner = jnp.sum(corner, axis=1, keepdims=True)
        ex_dy = jnp.where(lane == ny - 1, corner, pltpu.roll(ex, ny - 1, 1)) - ex
        p1 = ldx * row_psi[0, k] - lgx * ez
        p2 = ldx * row_psi[1, k] - lgx * ey
        p3 = hdy * row_psi[2, k] + hgy * ex_dy
        row_psi[0, k], row_psi[1, k], row_psi[2, k] = p1, p2, p3
        down_out[k, 0:size, :] = down_out[k, 0:size, :] - time_step * (ex_dz + ez - p1)
        down_out[k, size:2 * size, :] = down_out[k, size:2 * size, :] - time_step * (p2 - ey - ex_dy - p3)
    def below_side(k):
        ex, ey, ez = side_e[0, k], side_e[1, k], side_e[2, k]
        hdx, hgx, hdy, hgy = prof[0], prof[1], prof[12], prof[13]
        ex_dz = z_after(ex, side_e[0, k + 1]) - ex
        ex_dy = y_after(ex, first_y[0, k]) - ex
        p1 = hdx * side_psi[1, k] - hgx * ez
        p2 = hdx * side_psi[2, k] - hgx * ey
        p3 = hdy * side_psi[3, k] + hgy * ex_dy
        hy = side_h[1, k + 1] - side_step * (ex_dz + ez - p1)
        hz = side_h[2, k + 1] - side_step * (p2 - ey - ex_dy - p3)
        down_out[k, 2 * size:2 * size + 1, :] = hy[nx - 1:nx]
        down_out[k, 2 * size + 1:2 * size + 2, :] = hz[nx - 1:nx]

    def first_below(k):
        below_main(k)
        below_side(k)
        start(1, 0, k)

    def first_send(q, carry):
        y_each(lambda side, q: y_copy(side, True, q).wait_recv(), q)
        unpack(q)
        for i in range(2):
            k = 2 * q + i
            up_out[k, 2 * size:2 * size + 1, :] = side_e[1, k, 0:1, :]
            up_out[k, 2 * size + 1:2 * size + 2, :] = side_e[2, k, 0:1, :]
            start(0, 0, k)

        @pl.when(q > 0)
        def _():
            first_below(2 * q - 1)

        first_below(2 * q)
        return carry

    lax.fori_loop(0, chunks // 2, first_send, 0)
    first_below(chunks - 1)
    piece = n_modes // STEPS

    def mode_copies(s):
        return [
            pltpu.make_async_remote_copy(
                src_ref=basis_in.at[pl.ds(s * piece, piece), pl.ds(pl.multiple_of(peer * nx, nx), nx)],
                dst_ref=modes_3d.at[pl.ds(row * n_modes + s * piece, piece)],
                send_sem=mode_send.at[k, s], recv_sem=mode_recv.at[k, s],
                device_id={"row": peer, "col": col}, device_id_type=pl.DeviceIdType.MESH)
            for k, peer in enumerate(row_peers)
        ]

    def side_magnetic(slot, k):
        hdx, hgx = prof[0], prof[1]
        sdy, sgy = prof[12], prof[13]
        ex, ey, ez = side_e[0, k], side_e[1, k], side_e[2, k]
        row_y = spread(up_in[slot, k, 2 * size:2 * size + 1, :])
        row_z = spread(up_in[slot, k, 2 * size + 1:2 * size + 2, :])
        ey_dz = z_after(ey, side_e[1, k + 1]) - ey
        ex_dz = z_after(ex, side_e[0, k + 1]) - ex
        ez_dy = y_after(ez, first_y[1, k]) - ez
        ex_dy = y_after(ex, first_y[0, k]) - ex
        ez_dx = jnp.where(sub == nx - 1, row_z, pltpu.roll(ez, nx - 1, 0)) - ez
        ey_dx = jnp.where(sub == nx - 1, row_y, pltpu.roll(ey, nx - 1, 0)) - ey
        p0 = sdy * side_psi[0, k] + sgy * ez_dy
        p1 = hdx * side_psi[1, k] + hgx * ez_dx
        p2 = hdx * side_psi[2, k] + hgx * ey_dx
        p3 = sdy * side_psi[3, k] + sgy * ex_dy
        side_psi[0, k], side_psi[1, k], side_psi[2, k], side_psi[3, k] = p0, p1, p2, p3
        side_hx = side_h[0, k + 1] - side_step * (ez_dy + p0 - ey_dz)
        side_hy = side_h[1, k + 1] - side_step * (ex_dz - ez_dx - p1)
        side_hz = side_h[2, k + 1] - side_step * (ey_dx + p2 - ex_dy - p3)
        side_h[0, k + 1], side_h[1, k + 1], side_h[2, k + 1] = side_hx, side_hy, side_hz

    def tick(s, slot, k):
        more = s < STEPS - 1
        hdx, hgx, hdy, hgy = prof[0], prof[1], prof[2], prof[3]
        edx, egx, edy, egy = prof[4], prof[5], prof[6], prof[7]
        bdx, bgx = prof[8], prof[9]
        prior = jnp.where(k > 0, k - 1, chunks)
        wait_recv(0, slot, k)
        wait_recv(1, slot, k)
        wait_send(0, slot, k)

        @pl.when(k > 0)
        def _():
            wait_send(1, slot, k - 1)

        side_magnetic(slot, k)
        edge_ex, edge_ez = side_e[0, k], side_e[2, k]
        side_hx, side_hy, side_hz = side_h[0, k + 1], side_h[1, k + 1], side_h[2, k + 1]
        ey, ez = up_out[k, 0:size, :], up_out[k, size:2 * size, :]
        p1 = bdx * before_psi[0, k] + bgx * ez
        p2 = bdx * before_psi[1, k] + bgx * ey
        before_psi[0, k], before_psi[1, k] = p1, p2
        hy = before[0, k] + time_step * (ez + p1)
        hz = before[1, k] - time_step * (ey + p2)
        before[0, k], before[1, k] = hy, hz
        ey, ez = up_out[k, 2 * size:2 * size + 1, :], up_out[k, 2 * size + 1:2 * size + 2, :]
        factor = side_step[0:1] * (1.0 + bgx[0:1])
        before_h[0:size, :] = up_mask * (hy + down_in[slot, k, 0:size, :])
        before_h[size:2 * size, :] = up_mask * (hz + down_in[slot, k, size:2 * size, :])
        back_y = up_mask * (down_in[slot, k, 2 * size:2 * size + 1, :] + factor * ez)
        back_z = up_mask * (down_in[slot, k, 2 * size + 1:2 * size + 2, :] - factor * ey)

        last_hx, last_hz, first_ex, first_ez = zero, zero, zero, zero
        below_hx, below_hy = h_s[0, k * size], h_s[1, k * size]
        ex, ey, ez = e_s[0, k * size], e_s[1, k * size], e_s[2, k * size]
        for j in range(size):
            z = k * size + j
            next_ex, next_ey, next_ez = e_s[0, z + 1], e_s[1, z + 1], e_s[2, z + 1]
            row_y = spread(up_in[slot, k, j:j + 1, :])
            row_z = spread(up_in[slot, k, size + j:size + j + 1, :])
            to_end = (ny - 1 - half - width * j) % ny
            col_x = pltpu.roll(edge_ex, to_end, 1)
            col_z = pltpu.roll(edge_ez, to_end, 1)
            ey_dz = next_ey - ey
            ex_dz = next_ex - ex
            ez_dy = jnp.where(lane == ny - 1, col_z, pltpu.roll(ez, ny - 1, 1)) - ez
            ex_dy = jnp.where(lane == ny - 1, col_x, pltpu.roll(ex, ny - 1, 1)) - ex
            ez_dx = jnp.where(sub == nx - 1, row_z, pltpu.roll(ez, nx - 1, 0)) - ez
            ey_dx = jnp.where(sub == nx - 1, row_y, pltpu.roll(ey, nx - 1, 0)) - ey
            p0 = hdy * psi[0, z] + hgy * ez_dy
            p1 = hdx * psi[1, z] + hgx * ez_dx
            p2 = hdx * psi[2, z] + hgx * ey_dx
            p3 = hdy * psi[3, z] + hgy * ex_dy
            psi[0, z], psi[1, z], psi[2, z], psi[3, z] = p0, p1, p2, p3
            hx = h_s[0, z + 1] - time_step * (ez_dy + p0 - ey_dz)
            hy = h_s[1, z + 1] - time_step * (ex_dz - ez_dx - p1)
            hz = h_s[2, z + 1] - time_step * (ey_dx + p2 - ex_dy - p3)
            h_s[0, z + 1], h_s[1, z + 1], h_s[2, z + 1] = hx, hy, hz
            at = lane == half + width * j
            last_hx = jnp.where(at, pltpu.roll(hx, (half + width * j + 1) % ny, 1), last_hx)
            last_hz = jnp.where(at, pltpu.roll(hz, (half + width * j + 1) % ny, 1), last_hz)

            row_y = spread(before_h[j:j + 1, :])
            row_z = spread(before_h[size + j:size + j + 1, :])
            to_start = ny - (width * j + width - 1)
            col_x = pltpu.roll(side_hx, to_start, 1)
            col_z = pltpu.roll(side_hz, to_start, 1)
            hy_dz = hy - below_hy
            hx_dz = hx - below_hx
            hz_dy = hz - jnp.where(lane == 0, col_z, pltpu.roll(hz, 1, 1))
            hx_dy = hx - jnp.where(lane == 0, col_x, pltpu.roll(hx, 1, 1))
            hz_dx = hz - jnp.where(sub == 0, row_z, pltpu.roll(hz, 1, 0))
            hy_dx = hy - jnp.where(sub == 0, row_y, pltpu.roll(hy, 1, 0))
            p0 = edy * psi[4, z] + egy * hz_dy
            p1 = edx * psi[5, z] + egx * hz_dx
            p2 = edx * psi[6, z] + egx * hy_dx
            p3 = edy * psi[7, z] + egy * hx_dy
            psi[4, z], psi[5, z], psi[6, z], psi[7, z] = p0, p1, p2, p3
            amount = coef_s[z]
            ex = ex + amount * (hz_dy + p0 - hy_dz)
            ey = ey + amount * (hx_dz - hz_dx - p1)
            ez = ez + amount * (hy_dx + p2 - hx_dy - p3)
            e_s[0, z], e_s[1, z], e_s[2, z] = ex, ey, ez
            at = lane == width * j + width - 1
            first_ex = jnp.where(at, pltpu.roll(ex, width * j + width - 1, 1), first_ex)
            first_ez = jnp.where(at, pltpu.roll(ez, width * j + width - 1, 1), first_ez)
            up_out[k, j:j + 1, :] = ey[0:1]
            up_out[k, size + j:size + j + 1, :] = ez[0:1]
            for c, value in enumerate((ex, ey, ez)):
                last_x[c, k, j:j + 1, :] = value[nx - 1:nx]
            below_hx, below_hy = hx, hy
            ex, ey, ez = next_ex, next_ey, next_ez
        first_y[0, k] = first_ex
        first_y[1, k] = first_ez
        below_main(prior)

        sdy, sgy = prof[14], prof[15]
        hx, hy, hz = side_hx, side_hy, side_hz
        hy_dz = hy - z_before(hy, side_h[1, k])
        hx_dz = hx - z_before(hx, side_h[0, k])
        hz_dy = hz - y_before(hz, last_hz)
        hx_dy = hx - y_before(hx, last_hx)
        hz_dx = hz - jnp.where(sub == 0, spread(back_z), pltpu.roll(hz, 1, 0))
        hy_dx = hy - jnp.where(sub == 0, spread(back_y), pltpu.roll(hy, 1, 0))
        p0 = sdy * side_psi[4, k] + sgy * hz_dy
        p1 = edx * side_psi[5, k] + egx * hz_dx
        p2 = edx * side_psi[6, k] + egx * hy_dx
        p3 = sdy * side_psi[7, k] + sgy * hx_dy
        side_psi[4, k], side_psi[5, k], side_psi[6, k], side_psi[7, k] = p0, p1, p2, p3
        amount = side_coef[k]
        ex = side_e[0, k] + amount * (hz_dy + p0 - hy_dz)
        ey = side_e[1, k] + amount * (hx_dz - hz_dx - p1)
        ez = side_e[2, k] + amount * (hy_dx + p2 - hx_dy - p3)
        side_e[0, k], side_e[1, k], side_e[2, k] = ex, ey, ez
        up_out[k, 2 * size:2 * size + 1, :] = ey[0:1]
        up_out[k, 2 * size + 1:2 * size + 2, :] = ez[0:1]

        below_side(prior)

        @pl.when(more)
        def _():
            start(0, 1 - slot, k)

        @pl.when(jnp.logical_and(more, k > 0))
        def _():
            start(1, 1 - slot, k - 1)

    def step(s, carry):
        slot = lax.rem(s, 2)
        def body(k, carry):
            tick(s, slot, k)
            return carry

        lax.fori_loop(0, chunks, body, 0)
        wait_send(1, slot, chunks - 1)

        @pl.when(s < STEPS - 1)
        def _():
            below_main(chunks - 1)
            below_side(chunks - 1)
            start(1, 1 - slot, chunks - 1)

        @pl.when(s < STEPS - 1)
        def _():
            for copy in mode_copies(s):
                copy.start()

        @pl.when(s == STEPS - 2)
        def _():
            for copy in mode_copies(STEPS - 1):
                copy.start()

        return carry

    lax.fori_loop(0, STEPS, step, 0)
    def y_end(q, carry):
        y_each(lambda side, q: y_copy(side, False, q).wait_send(), q)
        return carry

    lax.fori_loop(0, nz // group, y_end, 0)

    count = snaps.shape[0] // nx

    def pick(s, carry):
        planes = []
        for j in range(8):
            index = index_ref[s * 8 + j]
            c = index // nz
            z = index - c * nz
            e_plane = e_s[jnp.minimum(c, 2), z]
            h_plane = h_s[jnp.maximum(c - 3, 0), z + 1]
            planes.append(jnp.where(c < 3, e_plane, h_plane))
        for j in range(8):
            snaps[pl.ds(pl.multiple_of((s * 8 + j) * nx, nx), nx), :] = planes[j]
        return carry

    lax.fori_loop(0, count // 8, pick, 0)
    load_b.wait()

    def wait_modes(s, carry):
        for copy in mode_copies(s):
            copy.wait()
        return carry

    lax.fori_loop(0, STEPS, wait_modes, 0)
    n_all = modes.shape[0] // nx
    dims = (((1,), (1,)), ((), ()))
    proj, gram = None, None
    for x in range(nx):
        a = snaps[pl.ds(x, count, stride=nx), :]
        b = modes[pl.ds(x, n_all, stride=nx), :]
        p = lax.dot_general(a, b, dims, precision=lax.Precision.HIGHEST, preferred_element_type=jnp.float32)
        g = lax.dot_general(a, a, dims, precision=lax.Precision.HIGHEST, preferred_element_type=jnp.float32)
        proj, gram = (p, g) if x == 0 else (proj + p, gram + g)
    gram = gram / float(nx * n_row * ny * n_col)
    share = count // (2 * n_row)
    fold = n_all // count
    short = share // fold
    for k in range(part.shape[0]):
        part[k, 0:share, :] = proj[k * share:(k + 1) * share]
        at = [k * share + m * short for m in range(fold)]
        part[k, share:share + short, :] = jnp.concatenate([gram[m:m + short] for m in at], axis=1)
    own = 2 * row + pair

    def exchange(peers, src_of, dst, sends, recvs):
        result = []
        for k, peer in enumerate(peers):
            result.append(pltpu.make_async_remote_copy(
                src_ref=src_of(peer), dst_ref=dst, send_sem=sends.at[k], recv_sem=recvs.at[k],
                device_id=peer, device_id_type=pl.DeviceIdType.MESH))
        for copy in result:
            copy.start()
        for copy in result:
            copy.wait()

    row_sums[own] = part[own]
    exchange(
        near, lambda peer: part.at[2 * peer["row"] + lax.rem(peer["col"], 2)],
        row_sums.at[own], sum_send, sum_recv)
    value = row_sums[0]
    for k in range(1, 2 * n_row):
        value = value + row_sums[k]
    level = lax.div(col, 2)
    col_sums[level] = value
    exchange(far, lambda peer: col_sums.at[level], col_sums.at[level], col_send, col_recv)
    value = col_sums[0]
    for k in range(1, n_col // 2):
        value = value + col_sums[k]
    total[own] = value
    exchange(near, lambda peer: total.at[own], total.at[own], back_send, back_recv)


def write_kernel(e_s, h_s, total, e_out, h_out, proj_out, gram_out, proj, gram, sems):
    nz = e_out.shape[1]
    copies = [
        pltpu.make_async_copy(e_s.at[:, pl.ds(0, nz)], e_out, sems.at[0]),
        pltpu.make_async_copy(h_s.at[:, pl.ds(1, nz)], h_out, sems.at[1]),
        pltpu.make_async_copy(proj, proj_out, sems.at[2]), pltpu.make_async_copy(gram, gram_out, sems.at[3]),
    ]
    copies[0].start()
    copies[1].start()
    n_all, count = proj.shape[1], gram.shape[1]
    share = count // total.shape[0]
    short = total.shape[1] - share
    for k in range(total.shape[0]):
        proj[k * share:(k + 1) * share, :] = total[k, 0:share, :]
        for m in range(n_all // count):
            at = k * share + m * short
            gram[at:at + short, :] = total[k, share:share + short, m * count:(m + 1) * count]
    copies[2].start()
    copies[3].start()
    for copy in copies:
        copy.wait()


def shards(e_field, h_field, e_coef, basis, pml_width, snap_index):
    nz, nx, ny = e_coef.shape
    n_row, n_col = lax.axis_size("row"), lax.axis_size("col")
    modes, count = basis.shape[0] * n_row, snap_index.shape[0]
    f32 = jnp.float32
    size = ny // STEPS // 2
    chunks = nz // size
    any_space = pl.BlockSpec(memory_space=pltpu.HBM)
    smem, vmem = pl.BlockSpec(memory_space=pltpu.SMEM), pl.BlockSpec(memory_space=pltpu.VMEM)
    held = pltpu.VMEM((3, nz + 1, nx, ny), f32)
    lines = count // (2 * n_row) * (modes + count) // modes
    e_s, h_s, total = pl.pallas_call(
        functools.partial(step_kernel, n_row, n_col),
        out_shape=[held, held, pltpu.VMEM((2 * n_row, lines, modes), f32)],
        in_specs=[smem, smem, any_space, any_space, any_space, any_space],
        out_specs=[vmem, vmem, vmem],
        scratch_shapes=[
            pltpu.VMEM((nz, nx, ny), f32), pltpu.VMEM((8, nz, nx, ny), f32),
            pltpu.VMEM((3, chunks + 2, nx, ny), f32), pltpu.VMEM((3, chunks + 2, nx, ny), f32),
            pltpu.VMEM((chunks, nx, ny), f32), pltpu.VMEM((8, chunks + 1, nx, ny), f32),
            pltpu.VMEM((2, chunks + 1, nx, ny), f32),
            pltpu.VMEM((2, chunks // 2, 7, nx, ny), f32), pltpu.VMEM((2, chunks // 2, 7, nx, ny), f32),
            pltpu.VMEM((chunks, 3 * size, ny), f32), pltpu.VMEM((2, chunks, 3 * size, ny), f32),
            pltpu.VMEM((chunks + 1, 3 * size, ny), f32), pltpu.VMEM((2, chunks, 3 * size, ny), f32),
            pltpu.VMEM((3, chunks + 2, size, ny), f32), pltpu.VMEM((3, chunks + 1, size, ny), f32),
            pltpu.VMEM((2, chunks, size, ny), f32), pltpu.VMEM((2, chunks, size, ny), f32),
            pltpu.VMEM((2 * size, ny), f32),
            pltpu.VMEM((16, nx, ny), f32),
            pltpu.VMEM((modes * nx, ny), f32), pltpu.VMEM((count * nx, ny), f32),
            pltpu.VMEM((2 * n_row, lines, modes), f32), pltpu.VMEM((2 * n_row, lines, modes), f32),
            pltpu.VMEM((n_col // 2, lines, modes), f32),
            pltpu.SemaphoreType.DMA((4,)),
            pltpu.SemaphoreType.DMA((2, chunks // 2)), pltpu.SemaphoreType.DMA((2, chunks // 2)),
            pltpu.SemaphoreType.DMA((2, 2, chunks)), pltpu.SemaphoreType.DMA((2, 2, chunks)),
            pltpu.SemaphoreType.DMA((n_row - 1, STEPS)), pltpu.SemaphoreType.DMA((n_row - 1, STEPS)),
            pltpu.SemaphoreType.DMA((2 * n_row - 1,)), pltpu.SemaphoreType.DMA((2 * n_row - 1,)),
            pltpu.SemaphoreType.DMA((n_col // 2 - 1,)), pltpu.SemaphoreType.DMA((n_col // 2 - 1,)),
            pltpu.SemaphoreType.DMA((2 * n_row - 1,)), pltpu.SemaphoreType.DMA((2 * n_row - 1,)),
        ],
        compiler_params=pltpu.CompilerParams(
            collective_id=0, has_side_effects=True, vmem_limit_bytes=65_280_000
        ),
    )(pml_width, snap_index, e_field, h_field, e_coef, basis)
    return pl.pallas_call(
        write_kernel,
        out_shape=[
            jax.ShapeDtypeStruct(e_field.shape, f32), jax.ShapeDtypeStruct(h_field.shape, f32),
            jax.ShapeDtypeStruct((count, modes), f32), jax.ShapeDtypeStruct((count, count), f32),
        ],
        in_specs=[vmem, vmem, vmem],
        out_specs=[any_space, any_space, any_space, any_space],
        scratch_shapes=[
            pltpu.VMEM((count, modes), f32), pltpu.VMEM((count, count), f32), pltpu.SemaphoreType.DMA((4,)),
        ],
        compiler_params=pltpu.CompilerParams(vmem_limit_bytes=16_777_216),
    )(e_s, h_s, total)


def solution(mesh):
    in_specs = (
        P(None, None, "row", "col"),
        P(None, None, "row", "col"),
        P(None, "row", "col"),
        P("row", None, "col"),
        P(),
        P(),
    )
    out_specs = (P(None, None, "row", "col"), P(None, None, "row", "col"), P(), P())
    return jax.shard_map(shards, mesh=mesh, in_specs=in_specs, out_specs=out_specs, check_vma=False)
```
